32 devices in a mesh: dp: 4 (over z), fsdp: 4 (over x, core), tensor: 2 (over y).
Axes of the slice: x: 2, y: 2, z: 4, core: 2. Of those that a mesh axis runs over, the one named last changes fastest.
Arguments:
- tokens: bfloat16 [4096, 8192], P(('dp', 'fsdp'), 'tensor'), may hold values from -700 to 700
- queries: bfloat16 [4096, 8192], P(('dp', 'fsdp'), 'tensor'), may hold values from -140 to 140
- segment_ids: int32 [32, 128], P(('dp', 'fsdp')), may hold values from 0 to 3, never falling along the last dimension, each value on 1 to 64 neighbouring positions
- gain: float32 [8192], P('tensor'), may hold values from 0.1 to 1.9
- key_value_weight: bfloat16 [8192, 2048], P('tensor', 'fsdp'), may hold values from -0.0625 to 0.0625
- plan: int32 [8], replicated, may hold values from 0 to 7, as said below
Outputs:
- attended: bfloat16 [4096, 8192], P(('dp', 'fsdp'), 'tensor')
The draws below stay inside these ranges and needn't reach their ends.
Inputs may be any that keep to these rules, and one draw needn't show every extreme that they name: plan is a permutation of 0 to 7; from one dp index to another at most 1 micro-batches go, and in every draw some pair of dp indices carries exactly 1.
All inputs are finite; a program needn't handle non-finite values.
Results may differ from the reference program's by a relative error of at most 0.011.
Values may be sent and summed in bfloat16 or wider, within the bound.
A program may use at most 64 MiB of HBM per device.

```python
import math
import jax
import jax.numpy as jnp
import numpy as np
from jax import lax

MODEL_WIDTH = 8192
QUERY_HEADS = 64
KEY_VALUE_HEADS = 8
HEAD_SIZE = 128
MICRO_TOKENS = 128
MB_DEV = 2
CAP = 1
MICRO = 8
BATCHES = 32
TOKENS = 4096
N_DP = 4
N_FSDP = 4


def draw_tokens(key, part):
    keys = jax.random.split(key, 3)
    columns = jnp.arange(MODEL_WIDTH, dtype=jnp.float32) / MODEL_WIDTH
    base = jnp.clip(jax.random.normal(keys[0], (TOKENS, MODEL_WIDTH), jnp.float32), -4.0, 4.0)
    ramp = jnp.sqrt(1.0 + 2.0 * columns)
    row_scale = jnp.exp(jax.random.uniform(keys[1], (TOKENS, 1), minval=0.0, maxval=math.log(10.0)))
    column_scale = jnp.exp(jax.random.uniform(keys[2], (1, MODEL_WIDTH), minval=0.0, maxval=math.log(10.0))) * ramp[None, :]
    return (base * row_scale * column_scale).astype(jnp.bfloat16)


def draw_queries(key, part):
    keys = jax.random.split(key, 1)
    values = jnp.clip(jax.random.normal(keys[0], (TOKENS, QUERY_HEADS * HEAD_SIZE), jnp.float32), -4.0, 4.0)
    return values.astype(jnp.bfloat16)


def draw_plan(key, part):
    keys = jax.random.split(key, 4)
    offsets = jax.random.permutation(keys[0], N_DP)
    arrangement = jax.random.permutation(keys[1], MB_DEV)
    shifting = offsets[arrangement // CAP]
    target_slot = jax.random.permutation(keys[2], MB_DEV)
    relabel = jax.random.permutation(keys[3], N_DP)
    relabel_back = jnp.argsort(relabel)
    sources = jnp.arange(N_DP, dtype=jnp.int32)
    target_rank = relabel[(relabel_back[sources][:, None] + shifting[None, :]) % N_DP]
    layout = target_rank * MB_DEV + target_slot[None, :]
    return layout.reshape(MICRO).astype(jnp.int32)


def block_levels(own_key, dims, pieces, smallest, high):
    def one(position, parts):
        heights = jax.random.uniform(jax.random.fold_in(jax.random.fold_in(own_key, 6), position), (parts,), jnp.float32, smallest / len(pieces), high / len(pieces))
        return jnp.repeat(jnp.exp(heights), dims[position] // parts).reshape((-1,) + (1,) * (len(dims) - position - 1))

    level = one(*pieces[0])
    for cut in pieces[1:]:
        level = level * one(*cut)
    return level


def profile(number_of, total, bound, skew):
    weights = [(1 << 20) // math.isqrt(standing ** skew) + 1 for standing in range(2, number_of + 1)]
    rest, counts = total - bound - (number_of - 1), [1] * (number_of - 1)
    while rest > 0:
        movable = [i for i in range(number_of - 1) if counts[i] < bound]
        whole, left = sum([weights[i] for i in movable]), rest
        for i in movable:
            addition = min(bound - counts[i], max(1, left * weights[i] // whole), rest)
            counts[i] = counts[i] + addition
            rest = rest - addition
    return np.array([bound] + counts)


def ragged(rng, count, total, most, skew):
    if count == 2:
        one = jax.random.randint(rng, (), max(1, total - most), min(most, total - 1) + 1)
        return jnp.stack([one, total - one])
    lengths = jnp.asarray(profile(count, total, most, skew), jnp.int32)
    couples = (count - 1) // 2
    source_of, taker = lengths[1:1 + 2 * couples:2], lengths[2:2 + 2 * couples:2]
    margin = jnp.minimum(source_of - 1, most - taker)
    moved = jax.random.randint(jax.random.fold_in(rng, 1), (couples,), 0, 1 << 20) % (margin + 1)
    lengths = lengths.at[1:1 + 2 * couples:2].set(source_of - moved).at[2:2 + 2 * couples:2].set(taker + moved)
    return lengths[jax.random.permutation(jax.random.fold_in(rng, 2), count)]


def noise(rng, extent, spread, limit, pieces=(), held_as=jnp.bfloat16):
    loudness = block_levels(rng, extent, pieces, -0.22, 0.18) if pieces else 1.0
    values = jax.random.normal(rng, extent, jnp.float32) * spread * loudness
    return jnp.minimum(jnp.maximum(values, -limit), limit).astype(held_as)


def setup_inputs(seed: int = 0) -> dict:
    key_of = jax.random.split(jax.random.key(seed), 7)
    tokens = draw_tokens(jax.random.fold_in(key_of[6], 71), 0)
    queries = draw_queries(jax.random.fold_in(key_of[6], 71), 0)
    segment_ids = jax.vmap(lambda own: jnp.searchsorted(jnp.cumsum(ragged(own, 4, MICRO_TOKENS, MICRO_TOKENS // 2, 1)), jnp.arange(MICRO_TOKENS), side="right"))(jax.random.split(key_of[2], BATCHES)).reshape((BATCHES, MICRO_TOKENS)).astype(jnp.int32)
    gain = jnp.clip(1.0 + 0.18 * jax.random.normal(key_of[3], (MODEL_WIDTH,), jnp.float32), 0.1, 1.9)
    key_value_weight = noise(key_of[4], (MODEL_WIDTH, 2 * KEY_VALUE_HEADS * HEAD_SIZE), MODEL_WIDTH ** -0.5, 0.0625, ((0, 2), (1, 4)))
    plan = draw_plan(jax.random.fold_in(key_of[6], 71), 0)
    return dict(tokens=tokens, queries=queries, segment_ids=segment_ids, gain=gain, key_value_weight=key_value_weight, plan=plan)


epsilon = 1e-05

def attend_block(query_block, key_block, value_block, doc_block):
    scores = jnp.einsum('qhgd,khd->hgqk', query_block, key_block, precision=lax.Precision.HIGHEST) * HEAD_SIZE ** (-0.5)
    positions = jnp.arange(MICRO_TOKENS, dtype=jnp.int32)
    allowed = (doc_block[:, None] == doc_block[None, :]) & (positions[:, None] >= positions[None, :])
    scores = jnp.where(allowed[None, None], scores, -1e+30)
    row_max = lax.optimization_barrier(jnp.max(scores, axis=-1, keepdims=True))
    expo = jnp.exp(scores - row_max)
    weights = (expo / lax.optimization_barrier(jnp.sum(expo, axis=-1, keepdims=True))).astype(jnp.bfloat16)
    mixed = jnp.einsum('hgqk,khd->qhgd', weights.astype(jnp.float32), value_block, precision=lax.Precision.HIGHEST)
    return mixed.reshape(MICRO_TOKENS, QUERY_HEADS * HEAD_SIZE).astype(jnp.bfloat16)

def reference(tokens, queries, segment_ids, gain, key_value_weight, plan):
    complete_weight = key_value_weight.astype(jnp.float32)
    head_group = QUERY_HEADS // KEY_VALUE_HEADS

    def one_block(item):
        rows, query_row_block, doc_row = item
        values = rows.astype(jnp.float32)
        scale = lax.rsqrt(lax.optimization_barrier(jnp.sum(values * values, axis=1)) / MODEL_WIDTH + epsilon)
        normed = (values * scale[:, None] * gain).astype(jnp.bfloat16)
        key_value_rows = jnp.dot(normed.astype(jnp.float32), complete_weight, precision=lax.Precision.HIGHEST)
        key_value_heads = key_value_rows.reshape(MICRO_TOKENS, KEY_VALUE_HEADS, 2, HEAD_SIZE)
        query_head_count = query_row_block.astype(jnp.float32).reshape(MICRO_TOKENS, KEY_VALUE_HEADS, head_group, HEAD_SIZE)
        return attend_block(query_head_count, key_value_heads[:, :, 0], key_value_heads[:, :, 1], doc_row)
    blocks = lax.map(one_block, (tokens.reshape(BATCHES, MICRO_TOKENS, MODEL_WIDTH), queries.reshape(BATCHES, MICRO_TOKENS, QUERY_HEADS * HEAD_SIZE), segment_ids))
    grid = blocks.reshape(N_DP, N_FSDP, MB_DEV, MICRO_TOKENS, QUERY_HEADS * HEAD_SIZE).transpose(1, 0, 2, 3, 4).reshape(N_FSDP, MICRO, MICRO_TOKENS, QUERY_HEADS * HEAD_SIZE)
    inverse = jnp.argsort(plan).astype(jnp.int32)
    moved = grid[:, inverse]
    return moved.reshape(N_FSDP, N_DP, MB_DEV, MICRO_TOKENS, QUERY_HEADS * HEAD_SIZE).transpose(1, 0, 2, 3, 4).reshape(TOKENS, QUERY_HEADS * HEAD_SIZE)
```

```python
import functools

import jax
import jax.numpy as jnp
from jax import lax
from jax.experimental import pallas as pl
from jax.experimental.pallas import tpu as pltpu
from jax.sharding import PartitionSpec as P


HEAD_SIZE = 128


epsilon = 1e-05


def pack_query_kernel(send_ref, query_ref, out_ref):
    out_ref[...] = query_ref[...]


def pack_queries(send_index, queries, length):
    ranks = send_index.shape[0]
    width = queries.shape[1]
    return pl.pallas_call(
        pack_query_kernel,
        grid_spec=pltpu.PrefetchScalarGridSpec(
            num_scalar_prefetch=1,
            grid=(ranks,),
            in_specs=[pl.BlockSpec((length, width), lambda r, send: (send[r], 0))],
            out_specs=pl.BlockSpec((length, width), lambda r, send: (r, 0)),
        ),
        out_shape=jax.ShapeDtypeStruct((ranks * length, width), queries.dtype),
        name="pack_queries",
    )(send_index, queries)


def split_partial_kernel(part_ref, out_ref):
    key = part_ref[:, :HEAD_SIZE]
    high = key.astype(jnp.bfloat16)
    out_ref[:, :HEAD_SIZE] = high
    out_ref[:, HEAD_SIZE : 2 * HEAD_SIZE] = (key - high.astype(jnp.float32)).astype(jnp.bfloat16)
    out_ref[:, 2 * HEAD_SIZE :] = part_ref[:, HEAD_SIZE:].astype(jnp.bfloat16)


def split_partial(partial_value, ranks, spread):
    rows, width = partial_value.shape
    all_heads = width // (2 * HEAD_SIZE)
    heads = all_heads // spread
    height = rows // ranks
    return pl.pallas_call(
        split_partial_kernel,
        grid=(spread, ranks, heads),
        in_specs=[pl.BlockSpec((height, 2 * HEAD_SIZE), lambda b, f, h: (f, b * heads + h))],
        out_specs=pl.BlockSpec(
            (height, 3 * HEAD_SIZE), lambda b, f, h: ((b * ranks + f) * heads + h, 0)
        ),
        out_shape=jax.ShapeDtypeStruct((ranks * all_heads * height, 3 * HEAD_SIZE), jnp.bfloat16),
        name="split_partial",
    )(partial_value)


def pack_kv_kernel(sources, send_ref, slot_ref, *refs):
    *part_refs, document_ref, out_ref = refs
    part_heads = part_refs[0].shape[1]
    heads_kv = part_heads * len(part_refs) // sources
    for h in range(heads_kv):
        first = h // part_heads * sources
        key = value = 0.0
        for part_ref in part_refs[first : first + sources]:
            block = part_ref[0, h % part_heads, 0].astype(jnp.float32)
            key += block[:, :HEAD_SIZE] + block[:, HEAD_SIZE : 2 * HEAD_SIZE]
            value += block[:, 2 * HEAD_SIZE :]
        high = key.astype(jnp.bfloat16)
        low = (key - high.astype(jnp.float32)).astype(jnp.bfloat16)
        for place, part in enumerate((high, low, value.astype(jnp.bfloat16))):
            start = (place * heads_kv + h) * HEAD_SIZE
            out_ref[:, start : start + HEAD_SIZE] = part
    out_ref[:, 3 * heads_kv * HEAD_SIZE :] = document_ref[...]


def pack_kv(send_index, slot_index, parts, documents, sources, length):
    ranks = send_index.shape[0]
    count = slot_index.shape[0]
    rows = documents.shape[0]
    part_heads = parts.shape[0] // (count * rows)
    packed = (3 * part_heads * count // sources + 1) * HEAD_SIZE

    def arrived(w):
        return pl.BlockSpec(
            (1, part_heads, 1, length, 3 * HEAD_SIZE),
            lambda r, send, slot: (slot[w], 0, send[r], 0, 0),
        )

    view = parts.reshape(count, part_heads, rows // length, length, 3 * HEAD_SIZE)
    return pl.pallas_call(
        functools.partial(pack_kv_kernel, sources),
        grid_spec=pltpu.PrefetchScalarGridSpec(
            num_scalar_prefetch=2,
            grid=(ranks,),
            in_specs=[arrived(w) for w in range(count)]
            + [pl.BlockSpec((length, HEAD_SIZE), lambda r, send, slot: (send[r], 0))],
            out_specs=pl.BlockSpec((length, packed), lambda r, send, slot: (r, 0)),
        ),
        out_shape=jax.ShapeDtypeStruct((ranks * length, packed), jnp.bfloat16),
        name="pack_kv",
    )(send_index, slot_index, *[view] * count, documents)


def attend_kernel(
    head_group, keep_ref, query_ref, high_ref, low_ref, value_ref, document_ref, out_ref
):
    length = query_ref.shape[0]
    query = jnp.concatenate(
        [query_ref[:, g * HEAD_SIZE : (g + 1) * HEAD_SIZE] for g in range(head_group)], axis=0
    )
    across = (((1,), (1,)), ((), ()))
    scores = lax.dot_general(query, high_ref[...], across, preferred_element_type=jnp.float32)
    scores += lax.dot_general(query, low_ref[...], across, preferred_element_type=jnp.float32)
    scores = (scores * HEAD_SIZE ** (-0.5)).reshape(head_group, length, length)
    document = document_ref[...].astype(jnp.float32)
    rows = lax.broadcasted_iota(jnp.int32, (length, length), 0)
    columns = lax.broadcasted_iota(jnp.int32, (length, length), 1)
    allowed = (document == document.T) & (columns <= rows)
    scores = jnp.where(allowed[None], scores, -1e30)
    row_max = jnp.max(scores, axis=-1, keepdims=True)
    expo = jnp.exp(scores - row_max)
    weights = (expo / jnp.sum(expo, axis=-1, keepdims=True)).astype(jnp.bfloat16)
    mixed = jnp.dot(
        weights.reshape(head_group * length, length),
        value_ref[...],
        preferred_element_type=jnp.float32,
    ).astype(jnp.bfloat16)
    for g in range(head_group):
        out_ref[:, g * HEAD_SIZE : (g + 1) * HEAD_SIZE] = mixed[g * length : (g + 1) * length]


def attend(keep_index, queries, packed, length):
    batches = keep_index.shape[0]
    heads_kv = (packed.shape[1] // HEAD_SIZE - 1) // 3
    width = queries.shape[1]
    group_width = width // heads_kv

    def part(place):
        return pl.BlockSpec(
            (length, HEAD_SIZE), lambda s, h, keep: (keep[s], place * heads_kv + h)
        )

    return pl.pallas_call(
        functools.partial(attend_kernel, group_width // HEAD_SIZE),
        grid_spec=pltpu.PrefetchScalarGridSpec(
            num_scalar_prefetch=1,
            grid=(batches, heads_kv),
            in_specs=[
                pl.BlockSpec((length, group_width), lambda s, h, keep: (keep[s], h)),
                part(0),
                part(1),
                part(2),
                pl.BlockSpec((length, HEAD_SIZE), lambda s, h, keep: (keep[s], 3 * heads_kv)),
            ],
            out_specs=pl.BlockSpec((length, group_width), lambda s, h, keep: (s, h)),
        ),
        out_shape=jax.ShapeDtypeStruct((batches * length, width), jnp.bfloat16),
        name="attend",
    )(keep_index, queries, packed, packed, packed, packed)


def project(rows, gain, key_value_weight):
    all_rows = lax.all_gather(rows, "fsdp", axis=0, tiled=True)
    values = rows.astype(jnp.float32)
    own_stats = jnp.sum(values * values, axis=1)
    stats = lax.psum(own_stats, "tensor")
    full_width = rows.shape[1] * lax.axis_size("tensor")
    scale = lax.all_gather(lax.rsqrt(stats / full_width + epsilon), "fsdp", axis=0, tiled=True)
    normed = (all_rows.astype(jnp.float32) * scale[:, None] * gain).astype(jnp.bfloat16)
    partial_value = jnp.dot(normed, key_value_weight, preferred_element_type=jnp.float32)
    f_ranks, t_ranks = lax.axis_size("fsdp"), lax.axis_size("tensor")
    joined, spread = max(1, f_ranks // t_ranks), max(1, t_ranks // f_ranks)
    count = f_ranks * spread
    parts = split_partial(partial_value, f_ranks, spread)
    share = parts.shape[0] // count
    f, t = lax.axis_index("fsdp"), lax.axis_index("tensor")
    number = f % joined * t_ranks + t
    arrived = []
    for p in range(count):
        pairs = []
        for i in range(f_ranks):
            for j in range(t_ranks):
                block = (i % joined * t_ranks + j + p) % count
                target = i // joined * spread + block // f_ranks
                pairs.append((i * t_ranks + j, block % f_ranks * t_ranks + target))
        sent = lax.dynamic_slice_in_dim(parts, (number + p) % count * share, share)
        arrived.append(lax.ppermute(sent, ("fsdp", "tensor"), pairs))
    slot_index = (t % spread * f_ranks + f - jnp.arange(count, dtype=jnp.int32)) % count
    return jnp.concatenate(arrived), slot_index


def shards(tokens, queries, segment_ids, gain, key_value_weight, plan):
    rank_count = lax.axis_size("dp")
    own_rank = lax.axis_index("dp")
    batches, length = segment_ids.shape
    own_dest = lax.dynamic_slice_in_dim(plan, own_rank * batches, batches) // batches
    rank_range = jnp.arange(rank_count, dtype=jnp.int32)
    slot_range = jnp.arange(batches, dtype=jnp.int32)
    send_index = jnp.sum(
        jnp.where(own_dest[None, :] == rank_range[:, None], slot_range[None, :], 0), axis=1
    )
    position = jnp.arange(plan.shape[0], dtype=jnp.int32)
    own_slots = own_rank * batches + slot_range
    keep_index = jnp.sum(
        jnp.where(plan[None, :] == own_slots[:, None], position[None, :] // batches, 0), axis=1
    )
    parcels = pack_queries(send_index, queries, length)
    moved_queries = lax.all_to_all(parcels, "dp", split_axis=0, concat_axis=0, tiled=True)
    documents = jnp.broadcast_to(
        segment_ids.reshape(batches * length, 1).astype(jnp.bfloat16),
        (batches * length, HEAD_SIZE),
    )
    parts, slot_index = project(tokens, gain, key_value_weight)
    packed = pack_kv(
        send_index, slot_index, parts, documents, lax.axis_size("tensor"), length
    )
    packed, moved_queries = lax.optimization_barrier((packed, moved_queries))
    moved_kv = lax.all_to_all(packed, "dp", split_axis=0, concat_axis=0, tiled=True)
    return attend(keep_index, moved_queries, moved_kv, length)


def route(plan, ranks, batches, slots, me, step):
    order = list(range(ranks))[::step]
    held = [jnp.int32(-1)] * slots
    transit = [jnp.int32(0)] * slots
    second = [jnp.int32(0)] * slots
    arrived = [jnp.int32(-1)] * slots
    for rank in order:
        here = me == rank
        arrived = [jnp.where(here, held[j], arrived[j]) for j in range(slots)]
        own = [plan[rank * batches + s] for s in range(batches)]
        beyond = lambda place: (step * (place // batches - rank) > 0) & (place >= 0)
        waiting = [beyond(place).astype(jnp.int32) for place in own]
        following = []
        for j in range(slots):
            passes = beyond(held[j]).astype(jnp.int32)
            first_fits = (1 - passes) * waiting[0]
            second_fits = (1 - passes) * (1 - first_fits) * waiting[1]
            waiting = [waiting[0] - first_fits, waiting[1] - second_fits]
            transit[j] = jnp.where(here, passes, transit[j])
            second[j] = jnp.where(here, second_fits, second[j])
            following.append(
                jnp.where(
                    passes > 0,
                    held[j],
                    jnp.where(first_fits > 0, own[0], jnp.where(second_fits > 0, own[1], -1)),
                )
            )
        held = following
    return transit, second, arrived


def pack_parts(part):
    key = part[:, :HEAD_SIZE]
    high = key.astype(jnp.bfloat16)
    low = (key - high.astype(jnp.float32)).astype(jnp.bfloat16)
    return jnp.concatenate([high, low, part[:, HEAD_SIZE:].astype(jnp.bfloat16)], axis=1)


def unpack_parts(packed):
    wide = packed.astype(jnp.float32)
    key = wide[:, :HEAD_SIZE] + wide[:, HEAD_SIZE : 2 * HEAD_SIZE]
    return jnp.concatenate([key, wide[:, 2 * HEAD_SIZE :]], axis=1)


def fused_kernel(
    slots,
    plan_ref,
    tokens_ref,
    query_ref,
    document_ref,
    gain_ref,
    weight_ref,
    out_ref,
    own_rows,
    far_rows,
    weight,
    stats_own,
    stats_far,
    scale_own,
    scale_far,
    query_own,
    query_in,
    query_out,
    documents,
    own_parts,
    far_parts,
    parts_a,
    parts_b,
    kv_own,
    kv_out,
    mixed,
    *rest,
):
    heads = parts_a.shape[0]
    kv_in = rest[:heads]
    (
        load_rows,
        load_weight,
        load_query,
        store_out,
        rows_send,
        rows_recv,
        weight_send,
        weight_recv,
        stats_send,
        stats_recv,
        scale_send,
        scale_recv,
        query_send,
        query_recv,
        document_send,
        document_recv,
        own_send,
        far_send,
        a_recv,
        b_recv,
        kv_send,
        kv_recv,
    ) = rest[heads:]
    ranks = lax.axis_size("dp")
    me, f, t = lax.axis_index("dp"), lax.axis_index("fsdp"), lax.axis_index("tensor")
    batches, length, depth = own_rows.shape
    chunks, _, _, chunk_width = query_own.shape
    core = f % 2
    side = f // 2
    far = f + 2 - 4 * side
    pair = f + 1 - 2 * core
    other = 1 - t
    off = side != t
    away = side == t
    rounds = range(chunks)
    first = jnp.where(2 * me < ranks, 0, 1)
    second_way = 1 - first

    def remote(src, dst, send, recv, device):
        return pltpu.make_async_remote_copy(
            src_ref=src,
            dst_ref=dst,
            send_sem=send,
            recv_sem=recv,
            device_id=device,
            device_id_type=pl.DeviceIdType.MESH,
        )

    rows_local = pltpu.make_async_copy(tokens_ref, own_rows, load_rows)
    rows_local.start()
    query_local = []
    for c in rounds:
        query_local.append(
            pltpu.make_async_copy(
                query_ref.at[:, :, pl.ds(c * chunk_width, chunk_width)],
                query_own.at[c],
                load_query.at[c],
            )
        )
        query_local[c].start()
    weight_local = pltpu.make_async_copy(weight_ref, weight.at[core], load_weight)
    weight_local.start()

    barrier = pltpu.get_barrier_semaphore()
    partners = [(me, far, t), (me, pair, t), (me, f, other), (me, far, other)]
    partners += [((me + k) % ranks, f, t) for k in range(1, ranks)]
    for partner in partners:
        pl.semaphore_signal(
            barrier, inc=1, device_id=partner, device_id_type=pl.DeviceIdType.MESH
        )
    pl.semaphore_wait(barrier, len(partners))

    rows_moves = [
        remote(
            tokens_ref.at[s], far_rows.at[s], rows_send.at[s], rows_recv.at[s], (me, far, t)
        )
        for s in range(batches)
    ]
    for move in rows_moves:
        move.start()
    weight_move = remote(
        weight_ref, weight.at[core], weight_send, weight_recv, (me, pair, t)
    )
    weight_move.start()
    weight_arrives = remote(
        weight_ref, weight.at[1 - core], weight_send, weight_recv, (me, pair, t)
    )

    for s in range(batches):
        line = document_ref[s : s + 1, :].astype(jnp.float32)
        documents[me, s] = jnp.broadcast_to(line, (8, length))

    plan = [plan_ref[i] for i in range(ranks * batches)]
    routes = [route(plan, ranks, batches, slots, me, step) for step in (1, -1)]

    def has_in(way):
        return jnp.where(way == 0, me > 0, me < ranks - 1)

    def has_out(way):
        return jnp.where(way == 0, me < ranks - 1, me > 0)

    def chosen(name, j, way):
        return jnp.where(way == 0, routes[0][name][j], routes[1][name][j])

    def onward(way):
        return (me + 1 - 2 * way, f, t)

    def query_copy(way, c):
        return remote(
            query_out.at[c, way],
            query_in.at[c, way],
            query_send.at[c, way],
            query_recv.at[c, way],
            onward(way),
        )

    def query_step(way, c):
        @pl.when(has_out(way))
        def _():
            @pl.when(has_in(way))
            def _():
                query_copy(way, c).wait_recv()

            for j in range(slots):
                own = jnp.where(
                    chosen(1, j, way) > 0, query_own[c, 1], query_own[c, 0]
                )
                query_out[c, way, j] = jnp.where(
                    chosen(0, j, way) > 0, query_in[c, way, j], own
                )
            query_copy(way, c).start()

    for move in query_local:
        move.wait()
    middle = (me > 0) & (me < ranks - 1)
    ends = (me == 0) | (me == ranks - 1)

    @pl.when(ends)
    def _():
        @pl.loop(0, chunks)
        def _(c):
            query_step(first, c)

    def query_round(c):
        @pl.when(middle)
        def _():
            query_step(first, c)
            if c:
                query_step(second_way, c - 1)
            if c == chunks - 1:
                query_step(second_way, c)

    document_moves = [
        remote(
            documents.at[me],
            documents.at[me],
            document_send.at[k - 1],
            document_recv.at[k - 1],
            ((me + k) % ranks, f, t),
        )
        for k in range(1, ranks)
    ]
    document_arrivals = [
        remote(
            documents.at[(me + ranks - k) % ranks],
            documents.at[(me + ranks - k) % ranks],
            document_send.at[k - 1],
            document_recv.at[k - 1],
            ((me + k) % ranks, f, t),
        )
        for k in range(1, ranks)
    ]
    for move in document_moves:
        move.start()

    rows_of = lax.broadcasted_iota(jnp.int32, (length, length), 0)
    columns_of = lax.broadcasted_iota(jnp.int32, (length, length), 1)
    diagonal = rows_of == columns_of
    block = 4 * HEAD_SIZE
    blocks = depth // block

    rows_local.wait()
    for s in range(batches):

        def squares(i, total, s=s):
            start = pl.multiple_of(i * block, block)
            values = own_rows[s, :, pl.ds(start, block)].astype(jnp.float32)
            values = values * values
            for g in range(block // HEAD_SIZE):
                total += values[:, g * HEAD_SIZE : (g + 1) * HEAD_SIZE]
            return total

        total = lax.fori_loop(
            0, blocks, squares, jnp.zeros((length, HEAD_SIZE), jnp.float32)
        )
        column = jnp.sum(total, axis=1, keepdims=True)
        line = jnp.sum(jnp.where(diagonal, column, 0.0), axis=0, keepdims=True)
        stats_own[s] = jnp.broadcast_to(line, (8, length))
    stats_move = remote(stats_own, stats_far, stats_send, stats_recv, (me, f, other))
    stats_move.start()
    stats_move.wait_recv()
    full_width = depth * lax.axis_size("tensor")
    scale_own[...] = lax.rsqrt((stats_own[...] + stats_far[...]) / full_width + epsilon)
    scale_move = remote(scale_own, scale_far, scale_send, scale_recv, (me, far, t))
    scale_move.start()

    def normalize(rows, scale, s):
        line = jnp.broadcast_to(scale[s, 0:1, :], (length, length))
        column = jnp.sum(jnp.where(diagonal, line, 0.0), axis=1, keepdims=True)

        @pl.loop(0, blocks)
        def _(i):
            start = pl.multiple_of(i * block, block)
            values = rows[s, :, pl.ds(start, block)].astype(jnp.float32)
            values = values * column * gain_ref[:, pl.ds(start, block)]
            rows[s, :, pl.ds(start, block)] = values.astype(jnp.bfloat16)

    for s in range(batches):
        normalize(own_rows, scale_own, s)

    def multiply(rows, h):
        half = heads // 2
        start = pl.multiple_of((h % half) * 2 * HEAD_SIZE, 2 * HEAD_SIZE)
        part = jnp.dot(
            rows[...].reshape(batches * length, depth),
            weight[h // half, :, pl.ds(start, 2 * HEAD_SIZE)],
            preferred_element_type=jnp.float32,
        )
        return pack_parts(part).reshape(batches, length, 3 * HEAD_SIZE)

    def own_copy(h):
        return remote(
            own_parts.at[h], parts_b.at[h], own_send.at[h], b_recv.at[h], (me, f, other)
        )

    def far_copy_a(h):
        return remote(
            far_parts.at[h], parts_a.at[h], far_send.at[h], a_recv.at[h], (me, far, t)
        )

    def far_copy_b(h):
        return remote(
            far_parts.at[h], parts_b.at[h], far_send.at[h], b_recv.at[h], (me, far, other)
        )

    def own_head(h):
        packed = multiply(own_rows, h)

        @pl.when(off)
        def _():
            own_parts[h] = packed
            own_copy(h).start()

        @pl.when(away)
        def _():
            parts_a[h] = packed

    def far_head(h):
        far_parts[h] = multiply(far_rows, h)

        @pl.when(off)
        def _():
            far_copy_b(h).start()

        @pl.when(away)
        def _():
            far_copy_a(h).start()

    query_round(0)
    weight_local.wait()
    weight_arrives.wait_recv()
    pl.loop(0, heads // 2)(own_head)
    query_round(1)
    pl.loop(heads // 2, heads)(own_head)

    def take_rows(s):
        rows_moves[s].wait_recv()
        if s == 0:
            scale_move.wait_recv()
        normalize(far_rows, scale_far, s)

    marks = [max(1, chunks // slots - 1), max(1, 2 * chunks // slots - 1)]
    for c in range(1, chunks):
        if c > 1:
            query_round(c)
        for s in range(batches):
            if marks[s] == c:
                take_rows(s)
        if marks[-1] == c:
            pl.loop(0, heads)(far_head)

    def kv_copy(way, h):
        return remote(
            kv_out.at[h, way],
            kv_in[h].at[way],
            kv_send.at[h, way],
            kv_recv.at[h, way],
            onward(way),
        )

    def kv_step(way, h):
        @pl.when(has_out(way))
        def _():
            @pl.when(has_in(way))
            def _():
                kv_copy(way, h).wait_recv()

            for j in range(slots):
                own = jnp.where(chosen(1, j, way) > 0, kv_own[h, 1], kv_own[h, 0])
                kv_out[h, way, j] = jnp.where(
                    chosen(0, j, way) > 0, kv_in[h][way, j], own
                )
            kv_copy(way, h).start()

    def join(h):
        @pl.when(off)
        def _():
            far_copy_a(h).wait_recv()

        far_copy_b(h).wait_recv()
        for s in range(batches):
            kv_own[h, s] = pack_parts(
                unpack_parts(parts_a[h, s]) + unpack_parts(parts_b[h, s])
            )

    per_head = chunks // heads
    group = per_head * chunk_width // HEAD_SIZE
    across = (((1,), (1,)), ((), ()))

    def place_of(s):
        want = me * batches + s
        own_at = jnp.int32(-1)
        for b in range(batches):
            for rank in range(ranks):
                hit = (me == rank) & (plan[rank * batches + b] == want)
                own_at = jnp.where(hit, b, own_at)
        in_at = []
        for way in range(2):
            at = jnp.int32(-1)
            for j in range(slots):
                at = jnp.where(routes[way][2][j] == want, j, at)
            in_at.append(at)
        source = jnp.int32(0)
        for b in range(ranks * batches):
            source = jnp.where(plan[b] == want, b, source)
        return own_at, in_at[0], in_at[1], source

    def pick(own, coming, places):
        own_at, right_at, left_at, _ = places
        value = jnp.where(
            right_at >= 0, coming(0, jnp.maximum(right_at, 0)), own(jnp.maximum(own_at, 0))
        )
        return jnp.where(left_at >= 0, coming(1, jnp.maximum(left_at, 0)), value)

    def out_copy(s, h):
        wide = group * HEAD_SIZE
        return pltpu.make_async_copy(
            mixed.at[s, h],
            out_ref.at[pl.ds(s * length, length), pl.ds(h * wide, wide)],
            store_out.at[s, h],
        )

    spots = [place_of(s) for s in range(batches)]

    def settle(copy, index):
        for way in range(2):

            @pl.when(has_in(way) & jnp.logical_not(has_out(way)))
            def _():
                copy(way, index).wait_recv()

    def attend_head(h):
        settle(kv_copy, h)

        @pl.loop(0, batches)
        def _(s):
            places = [jnp.where(s == 0, a, b) for a, b in zip(*spots)]
            tiles = []
            for c in range(h * per_head, (h + 1) * per_head):
                wide = pick(
                    lambda at: query_own[c, at], lambda way, at: query_in[c, way, at], places
                )
                for g in range(chunk_width // HEAD_SIZE):
                    tiles.append(wide[:, g * HEAD_SIZE : (g + 1) * HEAD_SIZE])
            query = jnp.concatenate(tiles, axis=0)
            kv = pick(lambda at: kv_own[h, at], lambda way, at: kv_in[h][way, at], places)
            high, low, value = (
                kv[:, i * HEAD_SIZE : (i + 1) * HEAD_SIZE] for i in range(3)
            )
            line = documents[places[3] // batches, places[3] % batches]
            line = jnp.broadcast_to(line[0:1, :], (length, length))
            scores = lax.dot_general(query, high, across, preferred_element_type=jnp.float32)
            scores += lax.dot_general(query, low, across, preferred_element_type=jnp.float32)
            scores = (scores * HEAD_SIZE ** (-0.5)).reshape(group, length, length)
            allowed = (line == line.T) & (columns_of <= rows_of)
            scores = jnp.where(allowed[None], scores, -1e30)
            row_max = jnp.max(scores, axis=-1, keepdims=True)
            expo = jnp.exp(scores - row_max)
            weights = (expo / jnp.sum(expo, axis=-1, keepdims=True)).astype(jnp.bfloat16)
            result = jnp.dot(
                weights.reshape(group * length, length),
                value,
                preferred_element_type=jnp.float32,
            ).astype(jnp.bfloat16)
            for g in range(group):
                mixed[s, h, :, g * HEAD_SIZE : (g + 1) * HEAD_SIZE] = result[
                    g * length : (g + 1) * length
                ]
            out_copy(s, h).start()

    for step in range(heads + 2):
        if step < heads:
            join(step)
            kv_step(first, step)
        if 1 <= step <= heads:
            kv_step(second_way, step - 1)
        if step == 1:
            for c in rounds:
                settle(query_copy, c)
            for move in document_arrivals:
                move.wait_recv()
        if step >= 2:
            attend_head(step - 2)

    for move in rows_moves + [weight_move, stats_move, scale_move] + document_moves:
        move.wait_send()
    for way in range(2):

        @pl.when(has_out(way))
        def _():
            for c in rounds:
                query_copy(way, c).wait_send()
            for h in range(heads):
                kv_copy(way, h).wait_send()

    for h in range(heads):

        @pl.when(off)
        def _():
            own_copy(h).wait_send()

        far_copy_a(h).wait_send()
        for s in range(batches):
            out_copy(s, h).wait()


def fused(slots, plan, tokens, queries, segment_ids, gain, key_value_weight):
    ranks = lax.axis_size("dp")
    batches, length = segment_ids.shape
    rows, depth = tokens.shape
    width = queries.shape[1]
    heads = 2 * key_value_weight.shape[1] // (2 * HEAD_SIZE)
    chunks = 2 * heads
    chunk_width = width // chunks
    packed = 3 * HEAD_SIZE
    bf16, f32 = jnp.bfloat16, jnp.float32
    dma = pltpu.SemaphoreType.DMA
    anywhere = pl.BlockSpec(memory_space=pl.ANY)
    return pl.pallas_call(
        functools.partial(fused_kernel, slots),
        out_shape=jax.ShapeDtypeStruct((rows, width), bf16),
        in_specs=[
            pl.BlockSpec(memory_space=pltpu.SMEM),
            anywhere,
            anywhere,
            pl.BlockSpec(memory_space=pltpu.VMEM),
            pl.BlockSpec(memory_space=pltpu.VMEM),
            anywhere,
        ],
        out_specs=anywhere,
        scratch_shapes=[
            pltpu.VMEM((batches, length, depth), bf16),
            pltpu.VMEM((batches, length, depth), bf16),
            pltpu.VMEM((2, depth, key_value_weight.shape[1]), bf16),
            pltpu.VMEM((batches, 8, length), f32),
            pltpu.VMEM((batches, 8, length), f32),
            pltpu.VMEM((batches, 8, length), f32),
            pltpu.VMEM((batches, 8, length), f32),
            pltpu.VMEM((chunks, batches, length, chunk_width), bf16),
            pltpu.VMEM((chunks, 2, slots, length, chunk_width), bf16),
            pltpu.VMEM((chunks, 2, slots, length, chunk_width), bf16),
            pltpu.VMEM((ranks, batches, 8, length), f32),
            pltpu.VMEM((heads, batches, length, packed), bf16),
            pltpu.VMEM((heads, batches, length, packed), bf16),
            pltpu.VMEM((heads, batches, length, packed), bf16),
            pltpu.VMEM((heads, batches, length, packed), bf16),
            pltpu.VMEM((heads, batches, length, packed), bf16),
            pltpu.VMEM((heads, 2, slots, length, packed), bf16),
            pltpu.VMEM((batches, heads, length, width // heads), bf16),
        ]
        + [pltpu.VMEM((2, slots, length, packed), bf16)] * heads
        + [
            dma,
            dma,
            dma((chunks,)),
            dma((batches, heads)),
            dma((batches,)),
            dma((batches,)),
            dma,
            dma,
            dma,
            dma,
            dma,
            dma,
            dma((chunks, 2)),
            dma((chunks, 2)),
            dma((ranks - 1,)),
            dma((ranks - 1,)),
            dma((heads,)),
            dma((heads,)),
            dma((heads,)),
            dma((heads,)),
            dma((heads, 2)),
            dma((heads, 2)),
        ],
        compiler_params=pltpu.CompilerParams(
            collective_id=slots, has_side_effects=True, vmem_limit_bytes=62 * 2**20
        ),
        name="fused",
    )(
        plan,
        tokens.reshape(batches, length, depth),
        queries.reshape(batches, length, width),
        segment_ids,
        gain.reshape(1, depth),
        key_value_weight,
    )


def fused_shards(tokens, queries, segment_ids, gain, key_value_weight, plan):
    batches = segment_ids.shape[0]
    most = batches * (lax.axis_size("dp") // 2)
    return fused(most, plan, tokens, queries, segment_ids, gain, key_value_weight)


def solution(mesh):
    placed = (
        P(("dp", "fsdp"), "tensor"),
        P(("dp", "fsdp"), "tensor"),
        P(("dp", "fsdp"), None),
        P("tensor"),
        P("tensor", "fsdp"),
        P(),
    )
    small = mesh.shape["tensor"] == 2 and mesh.shape["fsdp"] == 4 and mesh.shape["dp"] <= 4
    return jax.shard_map(
        fused_shards if small else shards,
        mesh=mesh,
        in_specs=placed,
        out_specs=P(("dp", "fsdp"), "tensor"),
        check_vma=False,
    )
```

```python
import functools

import jax
import jax.numpy as jnp
from jax import lax
from jax.experimental import pallas as pl
from jax.experimental.pallas import tpu as pltpu
from jax.sharding import PartitionSpec as P


HEAD_SIZE = 128


epsilon = 1e-05


def pack_query_kernel(send_ref, query_ref, out_ref):
    out_ref[...] = query_ref[...]


def pack_queries(send_index, queries, length):
    ranks = send_index.shape[0]
    width = queries.shape[1]
    return pl.pallas_call(
        pack_query_kernel,
        grid_spec=pltpu.PrefetchScalarGridSpec(
            num_scalar_prefetch=1,
            grid=(ranks,),
            in_specs=[pl.BlockSpec((length, width), lambda r, send: (send[r], 0))],
            out_specs=pl.BlockSpec((length, width), lambda r, send: (r, 0)),
        ),
        out_shape=jax.ShapeDtypeStruct((ranks * length, width), queries.dtype),
        name="pack_queries",
    )(send_index, queries)


def split_partial_kernel(part_ref, out_ref):
    key = part_ref[:, :HEAD_SIZE]
    high = key.astype(jnp.bfloat16)
    out_ref[:, :HEAD_SIZE] = high
    out_ref[:, HEAD_SIZE : 2 * HEAD_SIZE] = (key - high.astype(jnp.float32)).astype(jnp.bfloat16)
    out_ref[:, 2 * HEAD_SIZE :] = part_ref[:, HEAD_SIZE:].astype(jnp.bfloat16)


def split_partial(partial_value, ranks, spread):
    rows, width = partial_value.shape
    all_heads = width // (2 * HEAD_SIZE)
    heads = all_heads // spread
    height = rows // ranks
    return pl.pallas_call(
        split_partial_kernel,
        grid=(spread, ranks, heads),
        in_specs=[pl.BlockSpec((height, 2 * HEAD_SIZE), lambda b, f, h: (f, b * heads + h))],
        out_specs=pl.BlockSpec(
            (height, 3 * HEAD_SIZE), lambda b, f, h: ((b * ranks + f) * heads + h, 0)
        ),
        out_shape=jax.ShapeDtypeStruct((ranks * all_heads * height, 3 * HEAD_SIZE), jnp.bfloat16),
        name="split_partial",
    )(partial_value)


def pack_kv_kernel(sources, send_ref, slot_ref, *refs):
    *part_refs, document_ref, out_ref = refs
    part_heads = part_refs[0].shape[1]
    heads_kv = part_heads * len(part_refs) // sources
    for h in range(heads_kv):
        first = h // part_heads * sources
        key = value = 0.0
        for part_ref in part_refs[first : first + sources]:
            block = part_ref[0, h % part_heads, 0].astype(jnp.float32)
            key += block[:, :HEAD_SIZE] + block[:, HEAD_SIZE : 2 * HEAD_SIZE]
            value += block[:, 2 * HEAD_SIZE :]
        high = key.astype(jnp.bfloat16)
        low = (key - high.astype(jnp.float32)).astype(jnp.bfloat16)
        for place, part in enumerate((high, low, value.astype(jnp.bfloat16))):
            start = (place * heads_kv + h) * HEAD_SIZE
            out_ref[:, start : start + HEAD_SIZE] = part
    out_ref[:, 3 * heads_kv * HEAD_SIZE :] = document_ref[...]


def pack_kv(send_index, slot_index, parts, documents, sources, length):
    ranks = send_index.shape[0]
    count = slot_index.shape[0]
    rows = documents.shape[0]
    part_heads = parts.shape[0] // (count * rows)
    packed = (3 * part_heads * count // sources + 1) * HEAD_SIZE

    def arrived(w):
        return pl.BlockSpec(
            (1, part_heads, 1, length, 3 * HEAD_SIZE),
            lambda r, send, slot: (slot[w], 0, send[r], 0, 0),
        )

    view = parts.reshape(count, part_heads, rows // length, length, 3 * HEAD_SIZE)
    return pl.pallas_call(
        functools.partial(pack_kv_kernel, sources),
        grid_spec=pltpu.PrefetchScalarGridSpec(
            num_scalar_prefetch=2,
            grid=(ranks,),
            in_specs=[arrived(w) for w in range(count)]
            + [pl.BlockSpec((length, HEAD_SIZE), lambda r, send, slot: (send[r], 0))],
            out_specs=pl.BlockSpec((length, packed), lambda r, send, slot: (r, 0)),
        ),
        out_shape=jax.ShapeDtypeStruct((ranks * length, packed), jnp.bfloat16),
        name="pack_kv",
    )(send_index, slot_index, *[view] * count, documents)


def attend_kernel(
    head_group, keep_ref, query_ref, high_ref, low_ref, value_ref, document_ref, out_ref
):
    length = query_ref.shape[0]
    query = jnp.concatenate(
        [query_ref[:, g * HEAD_SIZE : (g + 1) * HEAD_SIZE] for g in range(head_group)], axis=0
    )
    across = (((1,), (1,)), ((), ()))
    scores = lax.dot_general(query, high_ref[...], across, preferred_element_type=jnp.float32)
    scores += lax.dot_general(query, low_ref[...], across, preferred_element_type=jnp.float32)
    scores = (scores * HEAD_SIZE ** (-0.5)).reshape(head_group, length, length)
    document = document_ref[...].astype(jnp.float32)
    rows = lax.broadcasted_iota(jnp.int32, (length, length), 0)
    columns = lax.broadcasted_iota(jnp.int32, (length, length), 1)
    allowed = (document == document.T) & (columns <= rows)
    scores = jnp.where(allowed[None], scores, -1e30)
    row_max = jnp.max(scores, axis=-1, keepdims=True)
    expo = jnp.exp(scores - row_max)
    weights = (expo / jnp.sum(expo, axis=-1, keepdims=True)).astype(jnp.bfloat16)
    mixed = jnp.dot(
        weights.reshape(head_group * length, length),
        value_ref[...],
        preferred_element_type=jnp.float32,
    ).astype(jnp.bfloat16)
    for g in range(head_group):
        out_ref[:, g * HEAD_SIZE : (g + 1) * HEAD_SIZE] = mixed[g * length : (g + 1) * length]


def attend(keep_index, queries, packed, length):
    batches = keep_index.shape[0]
    heads_kv = (packed.shape[1] // HEAD_SIZE - 1) // 3
    width = queries.shape[1]
    group_width = width // heads_kv

    def part(place):
        return pl.BlockSpec(
            (length, HEAD_SIZE), lambda s, h, keep: (keep[s], place * heads_kv + h)
        )

    return pl.pallas_call(
        functools.partial(attend_kernel, group_width // HEAD_SIZE),
        grid_spec=pltpu.PrefetchScalarGridSpec(
            num_scalar_prefetch=1,
            grid=(batches, heads_kv),
            in_specs=[
                pl.BlockSpec((length, group_width), lambda s, h, keep: (keep[s], h)),
                part(0),
                part(1),
                part(2),
                pl.BlockSpec((length, HEAD_SIZE), lambda s, h, keep: (keep[s], 3 * heads_kv)),
            ],
            out_specs=pl.BlockSpec((length, group_width), lambda s, h, keep: (s, h)),
        ),
        out_shape=jax.ShapeDtypeStruct((batches * length, width), jnp.bfloat16),
        name="attend",
    )(keep_index, queries, packed, packed, packed, packed)


def project(rows, gain, key_value_weight):
    all_rows = lax.all_gather(rows, "fsdp", axis=0, tiled=True)
    values = rows.astype(jnp.float32)
    own_stats = jnp.sum(values * values, axis=1)
    stats = lax.psum(own_stats, "tensor")
    full_width = rows.shape[1] * lax.axis_size("tensor")
    scale = lax.all_gather(lax.rsqrt(stats / full_width + epsilon), "fsdp", axis=0, tiled=True)
    normed = (all_rows.astype(jnp.float32) * scale[:, None] * gain).astype(jnp.bfloat16)
    partial_value = jnp.dot(normed, key_value_weight, preferred_element_type=jnp.float32)
    f_ranks, t_ranks = lax.axis_size("fsdp"), lax.axis_size("tensor")
    joined, spread = max(1, f_ranks // t_ranks), max(1, t_ranks // f_ranks)
    count = f_ranks * spread
    parts = split_partial(partial_value, f_ranks, spread)
    share = parts.shape[0] // count
    f, t = lax.axis_index("fsdp"), lax.axis_index("tensor")
    number = f % joined * t_ranks + t
    arrived = []
    for p in range(count):
        pairs = []
        for i in range(f_ranks):
            for j in range(t_ranks):
                block = (i % joined * t_ranks + j + p) % count
                target = i // joined * spread + block // f_ranks
                pairs.append((i * t_ranks + j, block % f_ranks * t_ranks + target))
        sent = lax.dynamic_slice_in_dim(parts, (number + p) % count * share, share)
        arrived.append(lax.ppermute(sent, ("fsdp", "tensor"), pairs))
    slot_index = (t % spread * f_ranks + f - jnp.arange(count, dtype=jnp.int32)) % count
    return jnp.concatenate(arrived), slot_index


def shards(tokens, queries, segment_ids, gain, key_value_weight, plan):
    rank_count = lax.axis_size("dp")
    own_rank = lax.axis_index("dp")
    batches, length = segment_ids.shape
    own_dest = lax.dynamic_slice_in_dim(plan, own_rank * batches, batches) // batches
    rank_range = jnp.arange(rank_count, dtype=jnp.int32)
    slot_range = jnp.arange(batches, dtype=jnp.int32)
    send_index = jnp.sum(
        jnp.where(own_dest[None, :] == rank_range[:, None], slot_range[None, :], 0), axis=1
    )
    position = jnp.arange(plan.shape[0], dtype=jnp.int32)
    own_slots = own_rank * batches + slot_range
    keep_index = jnp.sum(
        jnp.where(plan[None, :] == own_slots[:, None], position[None, :] // batches, 0), axis=1
    )
    parcels = pack_queries(send_index, queries, length)
    moved_queries = lax.all_to_all(parcels, "dp", split_axis=0, concat_axis=0, tiled=True)
    documents = jnp.broadcast_to(
        segment_ids.reshape(batches * length, 1).astype(jnp.bfloat16),
        (batches * length, HEAD_SIZE),
    )
    parts, slot_index = project(tokens, gain, key_value_weight)
    packed = pack_kv(
        send_index, slot_index, parts, documents, lax.axis_size("tensor"), length
    )
    packed, moved_queries = lax.optimization_barrier((packed, moved_queries))
    moved_kv = lax.all_to_all(packed, "dp", split_axis=0, concat_axis=0, tiled=True)
    return attend(keep_index, moved_queries, moved_kv, length)


def route(plan, ranks, batches, slots, me, step):
    order = list(range(ranks))[::step]
    held = [jnp.int32(-1)] * slots
    transit = [jnp.int32(0)] * slots
    second = [jnp.int32(0)] * slots
    arrived = [jnp.int32(-1)] * slots
    for rank in order:
        here = me == rank
        arrived = [jnp.where(here, held[j], arrived[j]) for j in range(slots)]
        own = [plan[rank * batches + s] for s in range(batches)]
        beyond = lambda place: (step * (place // batches - rank) > 0) & (place >= 0)
        waiting = [beyond(place).astype(jnp.int32) for place in own]
        following = []
        for j in range(slots):
            passes = beyond(held[j]).astype(jnp.int32)
            first_fits = (1 - passes) * waiting[0]
            second_fits = (1 - passes) * (1 - first_fits) * waiting[1]
            waiting = [waiting[0] - first_fits, waiting[1] - second_fits]
            transit[j] = jnp.where(here, passes, transit[j])
            second[j] = jnp.where(here, second_fits, second[j])
            following.append(
                jnp.where(
                    passes > 0,
                    held[j],
                    jnp.where(first_fits > 0, own[0], jnp.where(second_fits > 0, own[1], -1)),
                )
            )
        held = following
    return transit, second, arrived


def pack_parts(part):
    key = part[:, :HEAD_SIZE]
    high = key.astype(jnp.bfloat16)
    low = (key - high.astype(jnp.float32)).astype(jnp.bfloat16)
    return jnp.concatenate([high, low, part[:, HEAD_SIZE:].astype(jnp.bfloat16)], axis=1)


def unpack_parts(packed):
    wide = packed.astype(jnp.float32)
    key = wide[:, :HEAD_SIZE] + wide[:, HEAD_SIZE : 2 * HEAD_SIZE]
    return jnp.concatenate([key, wide[:, 2 * HEAD_SIZE :]], axis=1)


def fused_kernel(
    slots,
    plan_ref,
    tokens_ref,
    query_ref,
    document_ref,
    gain_ref,
    weight_ref,
    out_ref,
    own_rows,
    far_rows,
    weight,
    stats_own,
    stats_far,
    scale_own,
    scale_far,
    query_own,
    query_in,
    query_out,
    documents,
    own_parts,
    far_parts,
    parts_a,
    parts_b,
    kv_own,
    kv_out,
    mixed,
    *rest,
):
    heads = parts_a.shape[0]
    kv_in = rest[:heads]
    (
        load_rows,
        load_weight,
        load_query,
        store_out,
        rows_send,
        rows_recv,
        weight_send,
        weight_recv,
        stats_send,
        stats_recv,
        scale_send,
        scale_recv,
        query_send,
        query_recv,
        document_send,
        document_recv,
        own_send,
        far_send,
        a_recv,
        b_recv,
        kv_send,
        kv_recv,
    ) = rest[heads:]
    ranks = lax.axis_size("dp")
    me, f, t = lax.axis_index("dp"), lax.axis_index("fsdp"), lax.axis_index("tensor")
    batches, length, depth = own_rows.shape
    chunks, _, _, chunk_width = query_own.shape
    core = f % 2
    side = f // 2
    far = f + 2 - 4 * side
    pair = f + 1 - 2 * core
    other = 1 - t
    off = side != t
    away = side == t
    rounds = range(chunks)
    first = jnp.where(2 * me < ranks, 0, 1)
    second_way = 1 - first

    def remote(src, dst, send, recv, device):
        return pltpu.make_async_remote_copy(
            src_ref=src,
            dst_ref=dst,
            send_sem=send,
            recv_sem=recv,
            device_id=device,
            device_id_type=pl.DeviceIdType.MESH,
        )

    rows_local = pltpu.make_async_copy(tokens_ref, own_rows, load_rows)
    rows_local.start()
    query_local = []
    for c in rounds:
        query_local.append(
            pltpu.make_async_copy(
                query_ref.at[:, :, pl.ds(c * chunk_width, chunk_width)],
                query_own.at[c],
                load_query.at[c],
            )
        )
        query_local[c].start()
    weight_local = pltpu.make_async_copy(weight_ref, weight.at[core], load_weight)
    weight_local.start()

    barrier = pltpu.get_barrier_semaphore()
    partners = [(me, far, t), (me, pair, t), (me, f, other), (me, far, other)]
    partners += [((me + k) % ranks, f, t) for k in range(1, ranks)]
    for partner in partners:
        pl.semaphore_signal(
            barrier, inc=1, device_id=partner, device_id_type=pl.DeviceIdType.MESH
        )
    pl.semaphore_wait(barrier, len(partners))

    rows_moves = [
        remote(
            tokens_ref.at[s], far_rows.at[s], rows_send.at[s], rows_recv.at[s], (me, far, t)
        )
        for s in range(batches)
    ]
    for move in rows_moves:
        move.start()
    weight_move = remote(
        weight_ref, weight.at[core], weight_send, weight_recv, (me, pair, t)
    )
    weight_move.start()
    weight_arrives = remote(
        weight_ref, weight.at[1 - core], weight_send, weight_recv, (me, pair, t)
    )

    for s in range(batches):
        line = document_ref[s : s + 1, :].astype(jnp.float32)
        documents[me, s] = jnp.broadcast_to(line, (8, length))

    plan = [plan_ref[i] for i in range(ranks * batches)]
    routes = [route(plan, ranks, batches, slots, me, step) for step in (1, -1)]

    def has_in(way):
        return jnp.where(way == 0, me > 0, me < ranks - 1)

    def has_out(way):
        return jnp.where(way == 0, me < ranks - 1, me > 0)

    def chosen(name, j, way):
        return jnp.where(way == 0, routes[0][name][j], routes[1][name][j])

    def onward(way):
        return (me + 1 - 2 * way, f, t)

    def query_copy(way, c):
        return remote(
            query_out.at[c, way],
            query_in.at[c, way],
            query_send.at[c, way],
            query_recv.at[c, way],
            onward(way),
        )

    def query_step(way, c):
        @pl.when(has_out(way))
        def _():
            @pl.when(has_in(way))
            def _():
                query_copy(way, c).wait_recv()

            for j in range(slots):
                own = jnp.where(
                    chosen(1, j, way) > 0, query_own[c, 1], query_own[c, 0]
                )
                query_out[c, way, j] = jnp.where(
                    chosen(0, j, way) > 0, query_in[c, way, j], own
                )
            query_copy(way, c).start()

    for move in query_local:
        move.wait()
    middle = (me > 0) & (me < ranks - 1)
    ends = (me == 0) | (me == ranks - 1)

    @pl.when(ends)
    def _():
        @pl.loop(0, chunks)
        def _(c):
            query_step(first, c)

    def query_round(c):
        @pl.when(middle)
        def _():
            query_step(first, c)
            if c:
                query_step(second_way, c - 1)
            if c == chunks - 1:
                query_step(second_way, c)

    document_moves = [
        remote(
            documents.at[me],
            documents.at[me],
            document_send.at[k - 1],
            document_recv.at[k - 1],
            ((me + k) % ranks, f, t),
        )
        for k in range(1, ranks)
    ]
    document_arrivals = [
        remote(
            documents.at[(me + ranks - k) % ranks],
            documents.at[(me + ranks - k) % ranks],
            document_send.at[k - 1],
            document_recv.at[k - 1],
            ((me + k) % ranks, f, t),
        )
        for k in range(1, ranks)
    ]
    for move in document_moves:
        move.start()

    rows_of = lax.broadcasted_iota(jnp.int32, (length, length), 0)
    columns_of = lax.broadcasted_iota(jnp.int32, (length, length), 1)
    diagonal = rows_of == columns_of
    block = 4 * HEAD_SIZE
    blocks = depth // block

    rows_local.wait()
    for s in range(batches):

        def squares(i, total, s=s):
            start = pl.multiple_of(i * block, block)
            values = own_rows[s, :, pl.ds(start, block)].astype(jnp.float32)
            values = values * values
            for g in range(block // HEAD_SIZE):
                total += values[:, g * HEAD_SIZE : (g + 1) * HEAD_SIZE]
            return total

        total = lax.fori_loop(
            0, blocks, squares, jnp.zeros((length, HEAD_SIZE), jnp.float32)
        )
        column = jnp.sum(total, axis=1, keepdims=True)
        line = jnp.sum(jnp.where(diagonal, column, 0.0), axis=0, keepdims=True)
        stats_own[s] = jnp.broadcast_to(line, (8, length))
    stats_move = remote(stats_own, stats_far, stats_send, stats_recv, (me, f, other))
    stats_move.start()
    stats_move.wait_recv()
    full_width = depth * lax.axis_size("tensor")
    scale_own[...] = lax.rsqrt((stats_own[...] + stats_far[...]) / full_width + epsilon)
    scale_move = remote(scale_own, scale_far, scale_send, scale_recv, (me, far, t))
    scale_move.start()

    def normalize(rows, scale, s):
        line = jnp.broadcast_to(scale[s, 0:1, :], (length, length))
        column = jnp.sum(jnp.where(diagonal, line, 0.0), axis=1, keepdims=True)

        @pl.loop(0, blocks)
        def _(i):
            start = pl.multiple_of(i * block, block)
            values = rows[s, :, pl.ds(start, block)].astype(jnp.float32)
            values = values * column * gain_ref[:, pl.ds(start, block)]
            rows[s, :, pl.ds(start, block)] = values.astype(jnp.bfloat16)

    for s in range(batches):
        normalize(own_rows, scale_own, s)

    def multiply(rows, h):
        half = heads // 2
        start = pl.multiple_of((h % half) * 2 * HEAD_SIZE, 2 * HEAD_SIZE)
        part = jnp.dot(
            rows[...].reshape(batches * length, depth),
            weight[h // half, :, pl.ds(start, 2 * HEAD_SIZE)],
            preferred_element_type=jnp.float32,
        )
        return pack_parts(part).reshape(batches, length, 3 * HEAD_SIZE)

    def own_copy(h):
        return remote(
            own_parts.at[h], parts_b.at[h], own_send.at[h], b_recv.at[h], (me, f, other)
        )

    def far_copy_a(h):
        return remote(
            far_parts.at[h], parts_a.at[h], far_send.at[h], a_recv.at[h], (me, far, t)
        )

    def far_copy_b(h):
        return remote(
            far_parts.at[h], parts_b.at[h], far_send.at[h], b_recv.at[h], (me, far, other)
        )

    def own_head(h):
        packed = multiply(own_rows, h)

        @pl.when(off)
        def _():
            own_parts[h] = packed
            own_copy(h).start()

        @pl.when(away)
        def _():
            parts_a[h] = packed

    def far_head(h):
        far_parts[h] = multiply(far_rows, h)

        @pl.when(off)
        def _():
            far_copy_b(h).start()

        @pl.when(away)
        def _():
            far_copy_a(h).start()

    query_round(0)
    weight_local.wait()
    weight_arrives.wait_recv()
    pl.loop(0, heads // 2)(own_head)
    query_round(1)
    pl.loop(heads // 2, heads)(own_head)

    def take_rows(s):
        rows_moves[s].wait_recv()
        if s == 0:
            scale_move.wait_recv()
        normalize(far_rows, scale_far, s)

    marks = [max(1, chunks // slots - 1), max(1, 2 * chunks // slots - 1)]
    for c in range(1, chunks):
        if c > 1:
            query_round(c)
        for s in range(batches):
            if marks[s] == c:
                take_rows(s)
        if marks[-1] == c:
            pl.loop(0, heads)(far_head)

    def kv_copy(way, h):
        return remote(
            kv_out.at[h, way],
            kv_in[h].at[way],
            kv_send.at[h, way],
            kv_recv.at[h, way],
            onward(way),
        )

    def kv_step(way, h):
        @pl.when(has_out(way))
        def _():
            @pl.when(has_in(way))
            def _():
                kv_copy(way, h).wait_recv()

            for j in range(slots):
                own = jnp.where(chosen(1, j, way) > 0, kv_own[h, 1], kv_own[h, 0])
                kv_out[h, way, j] = jnp.where(
                    chosen(0, j, way) > 0, kv_in[h][way, j], own
                )
            kv_copy(way, h).start()

    def join(h):
        @pl.when(off)
        def _():
            far_copy_a(h).wait_recv()

        far_copy_b(h).wait_recv()
        for s in range(batches):
            kv_own[h, s] = pack_parts(
                unpack_parts(parts_a[h, s]) + unpack_parts(parts_b[h, s])
            )

    per_head = chunks // heads
    group = per_head * chunk_width // HEAD_SIZE
    across = (((1,), (1,)), ((), ()))

    def place_of(s):
        want = me * batches + s
        own_at = jnp.int32(-1)
        for b in range(batches):
            for rank in range(ranks):
                hit = (me == rank) & (plan[rank * batches + b] == want)
                own_at = jnp.where(hit, b, own_at)
        in_at = []
        for way in range(2):
            at = jnp.int32(-1)
            for j in range(slots):
                at = jnp.where(routes[way][2][j] == want, j, at)
            in_at.append(at)
        source = jnp.int32(0)
        for b in range(ranks * batches):
            source = jnp.where(plan[b] == want, b, source)
        return own_at, in_at[0], in_at[1], source

    def pick(own, coming, places):
        own_at, right_at, left_at, _ = places
        value = jnp.where(
            right_at >= 0, coming(0, jnp.maximum(right_at, 0)), own(jnp.maximum(own_at, 0))
        )
        return jnp.where(left_at >= 0, coming(1, jnp.maximum(left_at, 0)), value)

    def out_copy(s, h):
        wide = group * HEAD_SIZE
        return pltpu.make_async_copy(
            mixed.at[s, h],
            out_ref.at[pl.ds(s * length, length), pl.ds(h * wide, wide)],
            store_out.at[s, h],
        )

    spots = [place_of(s) for s in range(batches)]

    def settle(copy, index):
        for way in range(2):

            @pl.when(has_in(way) & jnp.logical_not(has_out(way)))
            def _():
                copy(way, index).wait_recv()

    def attend_head(h):
        settle(kv_copy, h)

        @pl.loop(0, batches)
        def _(s):
            places = [jnp.where(s == 0, a, b) for a, b in zip(*spots)]
            tiles = []
            for c in range(h * per_head, (h + 1) * per_head):
                wide = pick(
                    lambda at: query_own[c, at], lambda way, at: query_in[c, way, at], places
                )
                for g in range(chunk_width // HEAD_SIZE):
                    tiles.append(wide[:, g * HEAD_SIZE : (g + 1) * HEAD_SIZE])
            query = jnp.concatenate(tiles, axis=0)
            kv = pick(lambda at: kv_own[h, at], lambda way, at: kv_in[h][way, at], places)
            high, low, value = (
                kv[:, i * HEAD_SIZE : (i + 1) * HEAD_SIZE] for i in range(3)
            )
            line = documents[places[3] // batches, places[3] % batches]
            line = jnp.broadcast_to(line[0:1, :], (length, length))
            scores = lax.dot_general(query, high, across, preferred_element_type=jnp.float32)
            scores += lax.dot_general(query, low, across, preferred_element_type=jnp.float32)
            scores = (scores * HEAD_SIZE ** (-0.5)).reshape(group, length, length)
            allowed = (line == line.T) & (columns_of <= rows_of)
            scores = jnp.where(allowed[None], scores, -1e30)
            row_max = jnp.max(scores, axis=-1, keepdims=True)
            expo = jnp.exp(scores - row_max)
            weights = (expo / jnp.sum(expo, axis=-1, keepdims=True)).astype(jnp.bfloat16)
            result = jnp.dot(
                weights.reshape(group * length, length),
                value,
                preferred_element_type=jnp.float32,
            ).astype(jnp.bfloat16)
            for g in range(group):
                mixed[s, h, :, g * HEAD_SIZE : (g + 1) * HEAD_SIZE] = result[
                    g * length : (g + 1) * length
                ]
            out_copy(s, h).start()

    for step in range(heads + 2):
        if step < heads:
            join(step)
            kv_step(first, step)
        if 1 <= step <= heads:
            kv_step(second_way, step - 1)
        if step == 1:
            for c in rounds:
                settle(query_copy, c)
            for move in document_arrivals:
                move.wait_recv()
        if step >= 2:
            attend_head(step - 2)

    for move in rows_moves + [weight_move, stats_move, scale_move] + document_moves:
        move.wait_send()
    for way in range(2):

        @pl.when(has_out(way))
        def _():
            for c in rounds:
                query_copy(way, c).wait_send()
            for h in range(heads):
                kv_copy(way, h).wait_send()

    for h in range(heads):

        @pl.when(off)
        def _():
            own_copy(h).wait_send()

        far_copy_a(h).wait_send()
        for s in range(batches):
            out_copy(s, h).wait()


def fused(slots, plan, tokens, queries, segment_ids, gain, key_value_weight):
    ranks = lax.axis_size("dp")
    batches, length = segment_ids.shape
    rows, depth = tokens.shape
    width = queries.shape[1]
    heads = 2 * key_value_weight.shape[1] // (2 * HEAD_SIZE)
    chunks = 2 * heads
    chunk_width = width // chunks
    packed = 3 * HEAD_SIZE
    bf16, f32 = jnp.bfloat16, jnp.float32
    dma = pltpu.SemaphoreType.DMA
    anywhere = pl.BlockSpec(memory_space=pl.ANY)
    return pl.pallas_call(
        functools.partial(fused_kernel, slots),
        out_shape=jax.ShapeDtypeStruct((rows, width), bf16),
        in_specs=[
            pl.BlockSpec(memory_space=pltpu.SMEM),
            anywhere,
            anywhere,
            pl.BlockSpec(memory_space=pltpu.VMEM),
            pl.BlockSpec(memory_space=pltpu.VMEM),
            anywhere,
        ],
        out_specs=anywhere,
        scratch_shapes=[
            pltpu.VMEM((batches, length, depth), bf16),
            pltpu.VMEM((batches, length, depth), bf16),
            pltpu.VMEM((2, depth, key_value_weight.shape[1]), bf16),
            pltpu.VMEM((batches, 8, length), f32),
            pltpu.VMEM((batches, 8, length), f32),
            pltpu.VMEM((batches, 8, length), f32),
            pltpu.VMEM((batches, 8, length), f32),
            pltpu.VMEM((chunks, batches, length, chunk_width), bf16),
            pltpu.VMEM((chunks, 2, slots, length, chunk_width), bf16),
            pltpu.VMEM((chunks, 2, slots, length, chunk_width), bf16),
            pltpu.VMEM((ranks, batches, 8, length), f32),
            pltpu.VMEM((heads, batches, length, packed), bf16),
            pltpu.VMEM((heads, batches, length, packed), bf16),
            pltpu.VMEM((heads, batches, length, packed), bf16),
            pltpu.VMEM((heads, batches, length, packed), bf16),
            pltpu.VMEM((heads, batches, length, packed), bf16),
            pltpu.VMEM((heads, 2, slots, length, packed), bf16),
            pltpu.VMEM((batches, heads, length, width // heads), bf16),
        ]
        + [pltpu.VMEM((2, slots, length, packed), bf16)] * heads
        + [
            dma,
            dma,
            dma((chunks,)),
            dma((batches, heads)),
            dma((batches,)),
            dma((batches,)),
            dma,
            dma,
            dma,
            dma,
            dma,
            dma,
            dma((chunks, 2)),
            dma((chunks, 2)),
            dma((ranks - 1,)),
            dma((ranks - 1,)),
            dma((heads,)),
            dma((heads,)),
            dma((heads,)),
            dma((heads,)),
            dma((heads, 2)),
            dma((heads, 2)),
        ],
        compiler_params=pltpu.CompilerParams(
            collective_id=slots, has_side_effects=True, vmem_limit_bytes=62 * 2**20
        ),
        name="fused",
    )(
        plan,
        tokens.reshape(batches, length, depth),
        queries.reshape(batches, length, width),
        segment_ids,
        gain.reshape(1, depth),
        key_value_weight,
    )


def fused_shards(tokens, queries, segment_ids, gain, key_value_weight, plan):
    ranks = lax.axis_size("dp")
    batches = segment_ids.shape[0]
    target = plan // batches
    source = jnp.arange(plan.shape[0], dtype=jnp.int32) // batches
    cuts = jnp.arange(1, ranks, dtype=jnp.int32)[:, None]
    crossing = jnp.sum((source < cuts) & (target >= cuts), axis=1)
    most = batches * (ranks // 2)
    branches = [functools.partial(fused, slots) for slots in range(batches, most + 1)]
    index = jnp.clip(jnp.max(crossing) - batches, 0, most - batches)
    return lax.switch(
        index, branches, plan, tokens, queries, segment_ids, gain, key_value_weight
    )


def solution(mesh):
    placed = (
        P(("dp", "fsdp"), "tensor"),
        P(("dp", "fsdp"), "tensor"),
        P(("dp", "fsdp"), None),
        P("tensor"),
        P("tensor", "fsdp"),
        P(),
    )
    small = mesh.shape["tensor"] == 2 and mesh.shape["fsdp"] == 4 and mesh.shape["dp"] <= 4
    return jax.shard_map(
        fused_shards if small else shards,
        mesh=mesh,
        in_specs=placed,
        out_specs=P(("dp", "fsdp"), "tensor"),
        check_vma=False,
    )
```

```python
import functools

import jax
import jax.numpy as jnp
import numpy as np
from jax import lax
from jax.experimental import pallas as pl
from jax.experimental.pallas import tpu as pltpu
from jax.sharding import PartitionSpec as P


HEAD_SIZE = 128


epsilon = 1e-05


def pack_query_kernel(send_ref, query_ref, out_ref):
    out_ref[...] = query_ref[...]


def pack_queries(send_index, queries, length):
    ranks = send_index.shape[0]
    width = queries.shape[1]
    return pl.pallas_call(
        pack_query_kernel,
        grid_spec=pltpu.PrefetchScalarGridSpec(
            num_scalar_prefetch=1,
            grid=(ranks,),
            in_specs=[pl.BlockSpec((length, width), lambda r, send: (send[r], 0))],
            out_specs=pl.BlockSpec((length, width), lambda r, send: (r, 0)),
        ),
        out_shape=jax.ShapeDtypeStruct((ranks * length, width), queries.dtype),
        name="pack_queries",
    )(send_index, queries)


def split_partial_kernel(part_ref, out_ref):
    key = part_ref[:, :HEAD_SIZE]
    high = key.astype(jnp.bfloat16)
    out_ref[:, :HEAD_SIZE] = high
    out_ref[:, HEAD_SIZE : 2 * HEAD_SIZE] = (key - high.astype(jnp.float32)).astype(jnp.bfloat16)
    out_ref[:, 2 * HEAD_SIZE :] = part_ref[:, HEAD_SIZE:].astype(jnp.bfloat16)


def split_partial(partial_value, ranks, spread):
    rows, width = partial_value.shape
    all_heads = width // (2 * HEAD_SIZE)
    heads = all_heads // spread
    height = rows // ranks
    return pl.pallas_call(
        split_partial_kernel,
        grid=(spread, ranks, heads),
        in_specs=[pl.BlockSpec((height, 2 * HEAD_SIZE), lambda b, f, h: (f, b * heads + h))],
        out_specs=pl.BlockSpec(
            (height, 3 * HEAD_SIZE), lambda b, f, h: ((b * ranks + f) * heads + h, 0)
        ),
        out_shape=jax.ShapeDtypeStruct((ranks * all_heads * height, 3 * HEAD_SIZE), jnp.bfloat16),
        name="split_partial",
    )(partial_value)


def pack_kv_kernel(sources, send_ref, slot_ref, *refs):
    *part_refs, document_ref, out_ref = refs
    part_heads = part_refs[0].shape[1]
    heads_kv = part_heads * len(part_refs) // sources
    for h in range(heads_kv):
        first = h // part_heads * sources
        key = value = 0.0
        for part_ref in part_refs[first : first + sources]:
            block = part_ref[0, h % part_heads, 0].astype(jnp.float32)
            key += block[:, :HEAD_SIZE] + block[:, HEAD_SIZE : 2 * HEAD_SIZE]
            value += block[:, 2 * HEAD_SIZE :]
        high = key.astype(jnp.bfloat16)
        low = (key - high.astype(jnp.float32)).astype(jnp.bfloat16)
        for place, part in enumerate((high, low, value.astype(jnp.bfloat16))):
            start = (place * heads_kv + h) * HEAD_SIZE
            out_ref[:, start : start + HEAD_SIZE] = part
    out_ref[:, 3 * heads_kv * HEAD_SIZE :] = document_ref[...]


def pack_kv(send_index, slot_index, parts, documents, sources, length):
    ranks = send_index.shape[0]
    count = slot_index.shape[0]
    rows = documents.shape[0]
    part_heads = parts.shape[0] // (count * rows)
    packed = (3 * part_heads * count // sources + 1) * HEAD_SIZE

    def arrived(w):
        return pl.BlockSpec(
            (1, part_heads, 1, length, 3 * HEAD_SIZE),
            lambda r, send, slot: (slot[w], 0, send[r], 0, 0),
        )

    view = parts.reshape(count, part_heads, rows // length, length, 3 * HEAD_SIZE)
    return pl.pallas_call(
        functools.partial(pack_kv_kernel, sources),
        grid_spec=pltpu.PrefetchScalarGridSpec(
            num_scalar_prefetch=2,
            grid=(ranks,),
            in_specs=[arrived(w) for w in range(count)]
            + [pl.BlockSpec((length, HEAD_SIZE), lambda r, send, slot: (send[r], 0))],
            out_specs=pl.BlockSpec((length, packed), lambda r, send, slot: (r, 0)),
        ),
        out_shape=jax.ShapeDtypeStruct((ranks * length, packed), jnp.bfloat16),
        name="pack_kv",
    )(send_index, slot_index, *[view] * count, documents)


def attend_kernel(
    head_group, keep_ref, query_ref, high_ref, low_ref, value_ref, document_ref, out_ref
):
    length = query_ref.shape[0]
    query = jnp.concatenate(
        [query_ref[:, g * HEAD_SIZE : (g + 1) * HEAD_SIZE] for g in range(head_group)], axis=0
    )
    across = (((1,), (1,)), ((), ()))
    scores = lax.dot_general(query, high_ref[...], across, preferred_element_type=jnp.float32)
    scores += lax.dot_general(query, low_ref[...], across, preferred_element_type=jnp.float32)
    scores = (scores * HEAD_SIZE ** (-0.5)).reshape(head_group, length, length)
    document = document_ref[...].astype(jnp.float32)
    rows = lax.broadcasted_iota(jnp.int32, (length, length), 0)
    columns = lax.broadcasted_iota(jnp.int32, (length, length), 1)
    allowed = (document == document.T) & (columns <= rows)
    scores = jnp.where(allowed[None], scores, -1e30)
    row_max = jnp.max(scores, axis=-1, keepdims=True)
    expo = jnp.exp(scores - row_max)
    weights = (expo / jnp.sum(expo, axis=-1, keepdims=True)).astype(jnp.bfloat16)
    mixed = jnp.dot(
        weights.reshape(head_group * length, length),
        value_ref[...],
        preferred_element_type=jnp.float32,
    ).astype(jnp.bfloat16)
    for g in range(head_group):
        out_ref[:, g * HEAD_SIZE : (g + 1) * HEAD_SIZE] = mixed[g * length : (g + 1) * length]


def attend(keep_index, queries, packed, length):
    batches = keep_index.shape[0]
    heads_kv = (packed.shape[1] // HEAD_SIZE - 1) // 3
    width = queries.shape[1]
    group_width = width // heads_kv

    def part(place):
        return pl.BlockSpec(
            (length, HEAD_SIZE), lambda s, h, keep: (keep[s], place * heads_kv + h)
        )

    return pl.pallas_call(
        functools.partial(attend_kernel, group_width // HEAD_SIZE),
        grid_spec=pltpu.PrefetchScalarGridSpec(
            num_scalar_prefetch=1,
            grid=(batches, heads_kv),
            in_specs=[
                pl.BlockSpec((length, group_width), lambda s, h, keep: (keep[s], h)),
                part(0),
                part(1),
                part(2),
                pl.BlockSpec((length, HEAD_SIZE), lambda s, h, keep: (keep[s], 3 * heads_kv)),
            ],
            out_specs=pl.BlockSpec((length, group_width), lambda s, h, keep: (s, h)),
        ),
        out_shape=jax.ShapeDtypeStruct((batches * length, width), jnp.bfloat16),
        name="attend",
    )(keep_index, queries, packed, packed, packed, packed)


def project(rows, gain, key_value_weight):
    all_rows = lax.all_gather(rows, "fsdp", axis=0, tiled=True)
    values = rows.astype(jnp.float32)
    own_stats = jnp.sum(values * values, axis=1)
    stats = lax.psum(own_stats, "tensor")
    full_width = rows.shape[1] * lax.axis_size("tensor")
    scale = lax.all_gather(lax.rsqrt(stats / full_width + epsilon), "fsdp", axis=0, tiled=True)
    normed = (all_rows.astype(jnp.float32) * scale[:, None] * gain).astype(jnp.bfloat16)
    partial_value = jnp.dot(normed, key_value_weight, preferred_element_type=jnp.float32)
    f_ranks, t_ranks = lax.axis_size("fsdp"), lax.axis_size("tensor")
    joined, spread = max(1, f_ranks // t_ranks), max(1, t_ranks // f_ranks)
    count = f_ranks * spread
    parts = split_partial(partial_value, f_ranks, spread)
    share = parts.shape[0] // count
    f, t = lax.axis_index("fsdp"), lax.axis_index("tensor")
    number = f % joined * t_ranks + t
    arrived = []
    for p in range(count):
        pairs = []
        for i in range(f_ranks):
            for j in range(t_ranks):
                block = (i % joined * t_ranks + j + p) % count
                target = i // joined * spread + block // f_ranks
                pairs.append((i * t_ranks + j, block % f_ranks * t_ranks + target))
        sent = lax.dynamic_slice_in_dim(parts, (number + p) % count * share, share)
        arrived.append(lax.ppermute(sent, ("fsdp", "tensor"), pairs))
    slot_index = (t % spread * f_ranks + f - jnp.arange(count, dtype=jnp.int32)) % count
    return jnp.concatenate(arrived), slot_index


def shards(tokens, queries, segment_ids, gain, key_value_weight, plan):
    rank_count = lax.axis_size("dp")
    own_rank = lax.axis_index("dp")
    batches, length = segment_ids.shape
    own_dest = lax.dynamic_slice_in_dim(plan, own_rank * batches, batches) // batches
    rank_range = jnp.arange(rank_count, dtype=jnp.int32)
    slot_range = jnp.arange(batches, dtype=jnp.int32)
    send_index = jnp.sum(
        jnp.where(own_dest[None, :] == rank_range[:, None], slot_range[None, :], 0), axis=1
    )
    position = jnp.arange(plan.shape[0], dtype=jnp.int32)
    own_slots = own_rank * batches + slot_range
    keep_index = jnp.sum(
        jnp.where(plan[None, :] == own_slots[:, None], position[None, :] // batches, 0), axis=1
    )
    parcels = pack_queries(send_index, queries, length)
    moved_queries = lax.all_to_all(parcels, "dp", split_axis=0, concat_axis=0, tiled=True)
    documents = jnp.broadcast_to(
        segment_ids.reshape(batches * length, 1).astype(jnp.bfloat16),
        (batches * length, HEAD_SIZE),
    )
    parts, slot_index = project(tokens, gain, key_value_weight)
    packed = pack_kv(
        send_index, slot_index, parts, documents, lax.axis_size("tensor"), length
    )
    packed, moved_queries = lax.optimization_barrier((packed, moved_queries))
    moved_kv = lax.all_to_all(packed, "dp", split_axis=0, concat_axis=0, tiled=True)
    return attend(keep_index, moved_queries, moved_kv, length)


def route(plan, ranks, batches, slots, me, step):
    order = list(range(ranks))[::step]
    held = [jnp.int32(-1)] * slots
    transit = [jnp.int32(0)] * slots
    second = [jnp.int32(0)] * slots
    arrived = [jnp.int32(-1)] * slots
    for rank in order:
        here = me == rank
        arrived = [jnp.where(here, held[j], arrived[j]) for j in range(slots)]
        own = [plan[rank * batches + s] for s in range(batches)]
        beyond = lambda place: (step * (place // batches - rank) > 0) & (place >= 0)
        waiting = [beyond(place).astype(jnp.int32) for place in own]
        following = []
        for j in range(slots):
            passes = beyond(held[j]).astype(jnp.int32)
            first_fits = (1 - passes) * waiting[0]
            second_fits = (1 - passes) * (1 - first_fits) * waiting[1]
            waiting = [waiting[0] - first_fits, waiting[1] - second_fits]
            transit[j] = jnp.where(here, passes, transit[j])
            second[j] = jnp.where(here, second_fits, second[j])
            following.append(
                jnp.where(
                    passes > 0,
                    held[j],
                    jnp.where(first_fits > 0, own[0], jnp.where(second_fits > 0, own[1], -1)),
                )
            )
        held = following
    return transit, second, arrived


def pack_parts(part):
    key = part[:, :HEAD_SIZE]
    high = key.astype(jnp.bfloat16)
    low = (key - high.astype(jnp.float32)).astype(jnp.bfloat16)
    return jnp.concatenate([high, low, part[:, HEAD_SIZE:].astype(jnp.bfloat16)], axis=1)


def unpack_parts(packed):
    wide = packed.astype(jnp.float32)
    key = wide[:, :HEAD_SIZE] + wide[:, HEAD_SIZE : 2 * HEAD_SIZE]
    return jnp.concatenate([key, wide[:, 2 * HEAD_SIZE :]], axis=1)


def fused_kernel(
    slots,
    plan_ref,
    tokens_ref,
    query_ref,
    document_ref,
    gain_ref,
    weight_ref,
    out_ref,
    own_rows,
    far_rows,
    weight,
    stats_own,
    stats_far,
    scale_own,
    scale_far,
    query_own,
    query_in,
    query_out,
    documents,
    own_parts,
    far_parts,
    parts_a,
    parts_b,
    kv_own,
    kv_out,
    mixed,
    *rest,
):
    pieces = parts_a.shape[0]
    kv_in = rest[:pieces]
    (
        load_rows,
        load_weight,
        load_query,
        store_out,
        rows_send,
        rows_recv,
        weight_send,
        weight_recv,
        stats_send,
        stats_recv,
        scale_send,
        scale_recv,
        query_send,
        query_recv,
        document_send,
        document_recv,
        own_send,
        far_send,
        a_recv,
        b_recv,
        kv_send,
        kv_recv,
    ) = rest[pieces:]
    ranks = lax.axis_size("dp")
    me, f, t = lax.axis_index("dp"), lax.axis_index("fsdp"), lax.axis_index("tensor")
    batches, length, depth = own_rows.shape
    heads = mixed.shape[1]
    height = parts_a.shape[2]
    per_piece = pieces // heads
    tall = length // 4
    strips = batches * length // tall
    chunks, _, _, chunk_width = query_own.shape
    core = f % 2
    side = f // 2
    far = f + 2 - 4 * side
    pair = f + 1 - 2 * core
    other = 1 - t
    off = side != t
    away = side == t
    rounds = range(chunks)
    ahead = 2
    first = jnp.where(2 * me < ranks, 0, 1)
    second_way = 1 - first

    def remote(src, dst, send, recv, device):
        return pltpu.make_async_remote_copy(
            src_ref=src,
            dst_ref=dst,
            send_sem=send,
            recv_sem=recv,
            device_id=device,
            device_id_type=pl.DeviceIdType.MESH,
        )

    rows_local = pltpu.make_async_copy(tokens_ref, own_rows, load_rows)
    rows_local.start()
    query_local = []
    for c in rounds:
        query_local.append(
            pltpu.make_async_copy(
                query_ref.at[:, :, pl.ds(c * chunk_width, chunk_width)],
                query_own.at[c],
                load_query.at[c],
            )
        )
        query_local[c].start()
    weight_local = pltpu.make_async_copy(weight_ref, weight.at[core], load_weight)
    weight_local.start()

    barrier = pltpu.get_barrier_semaphore()
    partners = [(me, far, t), (me, pair, t), (me, f, other), (me, far, other)]
    partners += [((me + k) % ranks, f, t) for k in range(1, ranks)]
    for partner in partners:
        pl.semaphore_signal(
            barrier, inc=1, device_id=partner, device_id_type=pl.DeviceIdType.MESH
        )
    pl.semaphore_wait(barrier, len(partners))

    rows_moves = []
    for q in range(strips):
        part = (q * tall // length, pl.ds(q * tall % length, tall))
        rows_moves.append(
            remote(
                tokens_ref.at[part],
                far_rows.at[part],
                rows_send.at[q],
                rows_recv.at[q],
                (me, far, t),
            )
        )

    for move in rows_moves[:ahead]:
        move.start()
    weight_move = remote(
        weight_ref, weight.at[core], weight_send, weight_recv, (me, pair, t)
    )
    weight_move.start()
    weight_arrives = remote(
        weight_ref, weight.at[1 - core], weight_send, weight_recv, (me, pair, t)
    )

    for s in range(batches):
        line = document_ref[s : s + 1, :].astype(jnp.float32)
        documents[me, s] = jnp.broadcast_to(line, (8, length))

    document_moves = [
        remote(
            documents.at[me],
            documents.at[me],
            document_send.at[k - 1],
            document_recv.at[k - 1],
            ((me + k) % ranks, f, t),
        )
        for k in range(1, ranks)
    ]
    document_arrivals = [
        remote(
            documents.at[(me + ranks - k) % ranks],
            documents.at[(me + ranks - k) % ranks],
            document_send.at[k - 1],
            document_recv.at[k - 1],
            ((me + k) % ranks, f, t),
        )
        for k in range(1, ranks)
    ]
    for move in document_moves:
        move.start()

    plan = [plan_ref[i] for i in range(ranks * batches)]
    routes = [route(plan, ranks, batches, slots, me, step) for step in (1, -1)]

    def has_in(way):
        return jnp.where(way == 0, me > 0, me < ranks - 1)

    def has_out(way):
        return jnp.where(way == 0, me < ranks - 1, me > 0)

    def chosen(name, j, way):
        return jnp.where(way == 0, routes[0][name][j], routes[1][name][j])

    def onward(way):
        return (me + 1 - 2 * way, f, t)

    def query_copy(way, c):
        return remote(
            query_out.at[c, way],
            query_in.at[c, way],
            query_send.at[c, way],
            query_recv.at[c, way],
            onward(way),
        )

    def query_step(way, c):
        @pl.when(has_out(way))
        def _():
            @pl.when(has_in(way))
            def _():
                query_copy(way, c).wait_recv()

            for j in range(slots):
                own = jnp.where(
                    chosen(1, j, way) > 0, query_own[c, 1], query_own[c, 0]
                )
                query_out[c, way, j] = jnp.where(
                    chosen(0, j, way) > 0, query_in[c, way, j], own
                )
            query_copy(way, c).start()

    for move in query_local:
        move.wait()
    middle = (me > 0) & (me < ranks - 1)
    ends = (me == 0) | (me == ranks - 1)

    @pl.when(ends)
    def _():
        @pl.loop(0, chunks)
        def _(c):
            query_step(first, c)

    def query_round(c):
        @pl.when(middle)
        def _():
            if c < chunks:
                query_step(first, c)
            if c:
                query_step(second_way, c - 1)

    rows_of = lax.broadcasted_iota(jnp.int32, (length, length), 0)
    columns_of = lax.broadcasted_iota(jnp.int32, (length, length), 1)
    diagonal = rows_of == columns_of
    block = 4 * HEAD_SIZE
    blocks = depth // block

    rows_local.wait()
    for s in range(batches):

        def squares(i, total, s=s):
            start = pl.multiple_of(i * block, block)
            values = own_rows[s, :, pl.ds(start, block)].astype(jnp.float32)
            values = values * values
            for g in range(block // HEAD_SIZE):
                total += values[:, g * HEAD_SIZE : (g + 1) * HEAD_SIZE]
            return total

        total = lax.fori_loop(
            0, blocks, squares, jnp.zeros((length, HEAD_SIZE), jnp.float32)
        )
        column = jnp.sum(total, axis=1, keepdims=True)
        line = jnp.sum(jnp.where(diagonal, column, 0.0), axis=0, keepdims=True)
        stats_own[s] = jnp.broadcast_to(line, (8, length))
    stats_move = remote(stats_own, stats_far, stats_send, stats_recv, (me, f, other))
    stats_move.start()
    stats_move.wait_recv()
    full_width = depth * lax.axis_size("tensor")
    scale_own[...] = lax.rsqrt((stats_own[...] + stats_far[...]) / full_width + epsilon)
    scale_move = remote(scale_own, scale_far, scale_send, scale_recv, (me, far, t))
    scale_move.start()
    for move in rows_moves[ahead:]:
        move.start()

    def normalize(rows, scale, s, top, count):
        line = jnp.broadcast_to(scale[s, 0:1, :], (length, length))
        column = jnp.sum(jnp.where(diagonal, line, 0.0), axis=1, keepdims=True)
        column = column[top : top + count]

        @pl.loop(0, blocks)
        def _(i):
            start = pl.multiple_of(i * block, block)
            values = rows[s, top : top + count, pl.ds(start, block)].astype(jnp.float32)
            values = values * column * gain_ref[:, pl.ds(start, block)]
            rows[s, top : top + count, pl.ds(start, block)] = values.astype(jnp.bfloat16)

    for s in range(batches):
        normalize(own_rows, scale_own, s, 0, length)

    def multiply(rows, h):
        half = heads // 2
        start = pl.multiple_of((h % half) * 2 * HEAD_SIZE, 2 * HEAD_SIZE)
        part = jnp.dot(
            rows[...].reshape(batches * length, depth),
            weight[h // half, :, pl.ds(start, 2 * HEAD_SIZE)],
            preferred_element_type=jnp.float32,
        )
        return pack_parts(part).reshape(batches, length, 3 * HEAD_SIZE)

    def own_copy(i):
        return remote(
            own_parts.at[i], parts_b.at[i], own_send.at[i], b_recv.at[i], (me, f, other)
        )

    def far_copy_a(i):
        return remote(
            far_parts.at[i], parts_a.at[i], far_send.at[i], a_recv.at[i], (me, far, t)
        )

    def far_copy_b(i):
        return remote(
            far_parts.at[i], parts_b.at[i], far_send.at[i], b_recv.at[i], (me, far, other)
        )

    def own_head(h):
        packed = multiply(own_rows, h)
        for j in range(per_piece):
            i = h * per_piece + j
            piece = packed[:, j * height : (j + 1) * height]

            @pl.when(off)
            def _():
                own_parts[i] = piece
                own_copy(i).start()

            @pl.when(away)
            def _():
                parts_a[i] = piece

    def far_head(h):
        packed = multiply(far_rows, h)
        for j in range(per_piece):
            far_parts[h * per_piece + j] = packed[:, j * height : (j + 1) * height]

    def send_far(i):
        if i % per_piece == 0:
            far_head(i // per_piece)

        @pl.when(off)
        def _():
            far_copy_b(i).start()

        @pl.when(away)
        def _():
            far_copy_a(i).start()

    def take_rows(q):
        rows_moves[q].wait_recv()
        if q == 0:
            scale_move.wait_recv()
        normalize(far_rows, scale_far, q * tall // length, q * tall % length, tall)

    taken = 0
    later = list(range(chunks + 1))
    while taken < strips:
        c = later.pop(0)
        query_round(c)
        paced = (c + 1) * slots * length * chunk_width // (tall * depth)
        if c == 0:
            weight_local.wait()
            weight_arrives.wait_recv()
        if c < 2:
            pl.loop(c * heads // 2, (c + 1) * heads // 2)(own_head)
        upto = paced
        if (c + 2) * slots * length * chunk_width >= strips * tall * depth:
            upto = strips
        while taken < upto:
            take_rows(taken)
            taken += 1

    def kv_copy(way, h):
        return remote(
            kv_out.at[h, way],
            kv_in[h].at[way],
            kv_send.at[h, way],
            kv_recv.at[h, way],
            onward(way),
        )

    def kv_step(way, h):
        @pl.when(has_out(way))
        def _():
            @pl.when(has_in(way))
            def _():
                kv_copy(way, h).wait_recv()

            for j in range(slots):
                own = jnp.where(chosen(1, j, way) > 0, kv_own[h, 1], kv_own[h, 0])
                kv_out[h, way, j] = jnp.where(
                    chosen(0, j, way) > 0, kv_in[h][way, j], own
                )
            kv_copy(way, h).start()

    def join(h):
        @pl.when(off)
        def _():
            far_copy_a(h).wait_recv()

        far_copy_b(h).wait_recv()
        for s in range(batches):
            kv_own[h, s] = pack_parts(
                unpack_parts(parts_a[h, s]) + unpack_parts(parts_b[h, s])
            )

    per_head = chunks // heads
    group = per_head * chunk_width // HEAD_SIZE
    across = (((1,), (1,)), ((), ()))

    def place_of(s):
        want = me * batches + s
        own_at = jnp.int32(-1)
        for b in range(batches):
            for rank in range(ranks):
                hit = (me == rank) & (plan[rank * batches + b] == want)
                own_at = jnp.where(hit, b, own_at)
        in_at = []
        for way in range(2):
            at = jnp.int32(-1)
            for j in range(slots):
                at = jnp.where(routes[way][2][j] == want, j, at)
            in_at.append(at)
        source = jnp.int32(0)
        for b in range(ranks * batches):
            source = jnp.where(plan[b] == want, b, source)
        return own_at, in_at[0], in_at[1], source

    def pick(own, coming, places):
        own_at, right_at, left_at, _ = places
        value = jnp.where(
            right_at >= 0, coming(0, jnp.maximum(right_at, 0)), own(jnp.maximum(own_at, 0))
        )
        return jnp.where(left_at >= 0, coming(1, jnp.maximum(left_at, 0)), value)

    def out_copy(s, h):
        wide = group * HEAD_SIZE
        return pltpu.make_async_copy(
            mixed.at[s, h],
            out_ref.at[pl.ds(s * length, length), pl.ds(h * wide, wide)],
            store_out.at[s, h],
        )

    spots = [place_of(s) for s in range(batches)]

    def settle(copy, index):
        for way in range(2):

            @pl.when(has_in(way) & jnp.logical_not(has_out(way)))
            def _():
                copy(way, index).wait_recv()

    def attend_head(h):
        for i in range(h * per_piece, (h + 1) * per_piece):
            settle(kv_copy, i)

        @pl.loop(0, batches)
        def _(s):
            places = [jnp.where(s == 0, a, b) for a, b in zip(*spots)]
            tiles = []
            for c in range(h * per_head, (h + 1) * per_head):
                wide = pick(
                    lambda at: query_own[c, at], lambda way, at: query_in[c, way, at], places
                )
                for g in range(chunk_width // HEAD_SIZE):
                    tiles.append(wide[:, g * HEAD_SIZE : (g + 1) * HEAD_SIZE])
            query = jnp.concatenate(tiles, axis=0)
            kv = jnp.concatenate(
                [
                    pick(lambda at: kv_own[i, at], lambda way, at: kv_in[i][way, at], places)
                    for i in range(h * per_piece, (h + 1) * per_piece)
                ],
                axis=0,
            )
            high, low, value = (
                kv[:, i * HEAD_SIZE : (i + 1) * HEAD_SIZE] for i in range(3)
            )
            line = documents[places[3] // batches, places[3] % batches]
            line = jnp.broadcast_to(line[0:1, :], (length, length))
            scores = lax.dot_general(query, high, across, preferred_element_type=jnp.float32)
            scores += lax.dot_general(query, low, across, preferred_element_type=jnp.float32)
            scores = (scores * HEAD_SIZE ** (-0.5)).reshape(group, length, length)
            allowed = (line == line.T) & (columns_of <= rows_of)
            scores = jnp.where(allowed[None], scores, -1e30)
            row_max = jnp.max(scores, axis=-1, keepdims=True)
            expo = jnp.exp(scores - row_max)
            weights = (expo / jnp.sum(expo, axis=-1, keepdims=True)).astype(jnp.bfloat16)
            result = jnp.dot(
                weights.reshape(group * length, length),
                value,
                preferred_element_type=jnp.float32,
            ).astype(jnp.bfloat16)
            for g in range(group):
                mixed[s, h, :, g * HEAD_SIZE : (g + 1) * HEAD_SIZE] = result[
                    g * length : (g + 1) * length
                ]
            out_copy(s, h).start()

    for i in range(pieces):
        send_far(i)
        if i == per_piece - 1 and len(later) > 1:
            query_round(later.pop(0))
    while len(later) > 1:
        query_round(later.pop(0))
    for step in range(pieces + 1):
        if step < pieces:
            join(step)
            kv_step(first, step)
        if step == 1:
            query_round(later.pop(0))
            for c in rounds:
                settle(query_copy, c)
            for move in document_arrivals:
                move.wait_recv()
        if step >= 2:
            kv_step(second_way, step - 2)
        if step == pieces:
            kv_step(second_way, step - 1)
        if step == pieces:
            for h in range(heads):
                attend_head(h)

    for move in rows_moves + [weight_move, stats_move, scale_move] + document_moves:
        move.wait_send()
    for way in range(2):

        @pl.when(has_out(way))
        def _():
            for c in rounds:
                query_copy(way, c).wait_send()
            for i in range(pieces):
                kv_copy(way, i).wait_send()

    for i in range(pieces):

        @pl.when(off)
        def _():
            own_copy(i).wait_send()

        far_copy_a(i).wait_send()
    for h in range(heads):
        for s in range(batches):
            out_copy(s, h).wait()


def fused(slots, plan, tokens, queries, segment_ids, gain, key_value_weight):
    ranks = lax.axis_size("dp")
    batches, length = segment_ids.shape
    rows, depth = tokens.shape
    width = queries.shape[1]
    heads = 2 * key_value_weight.shape[1] // (2 * HEAD_SIZE)
    chunks = 2 * heads
    chunk_width = width // chunks
    pieces = 2 * heads
    packed = (length // 2, 3 * HEAD_SIZE)
    bf16, f32 = jnp.bfloat16, jnp.float32
    dma = pltpu.SemaphoreType.DMA
    anywhere = pl.BlockSpec(memory_space=pl.ANY)
    return pl.pallas_call(
        functools.partial(fused_kernel, slots),
        out_shape=jax.ShapeDtypeStruct((rows, width), bf16),
        in_specs=[
            pl.BlockSpec(memory_space=pltpu.SMEM),
            anywhere,
            anywhere,
            pl.BlockSpec(memory_space=pltpu.VMEM),
            pl.BlockSpec(memory_space=pltpu.VMEM),
            anywhere,
        ],
        out_specs=anywhere,
        scratch_shapes=[
            pltpu.VMEM((batches, length, depth), bf16),
            pltpu.VMEM((batches, length, depth), bf16),
            pltpu.VMEM((2, depth, key_value_weight.shape[1]), bf16),
            pltpu.VMEM((batches, 8, length), f32),
            pltpu.VMEM((batches, 8, length), f32),
            pltpu.VMEM((batches, 8, length), f32),
            pltpu.VMEM((batches, 8, length), f32),
            pltpu.VMEM((chunks, batches, length, chunk_width), bf16),
            pltpu.VMEM((chunks, 2, slots, length, chunk_width), bf16),
            pltpu.VMEM((chunks, 2, slots, length, chunk_width), bf16),
            pltpu.VMEM((ranks, batches, 8, length), f32),
            pltpu.VMEM((pieces, batches, *packed), bf16),
            pltpu.VMEM((pieces, batches, *packed), bf16),
            pltpu.VMEM((pieces, batches, *packed), bf16),
            pltpu.VMEM((pieces, batches, *packed), bf16),
            pltpu.VMEM((pieces, batches, *packed), bf16),
            pltpu.VMEM((pieces, 2, slots, *packed), bf16),
            pltpu.VMEM((batches, heads, length, width // heads), bf16),
        ]
        + [pltpu.VMEM((2, slots, *packed), bf16)] * pieces
        + [
            dma,
            dma,
            dma((chunks,)),
            dma((batches, heads)),
            dma((4 * batches,)),
            dma((4 * batches,)),
            dma,
            dma,
            dma,
            dma,
            dma,
            dma,
            dma((chunks, 2)),
            dma((chunks, 2)),
            dma((ranks - 1,)),
            dma((ranks - 1,)),
            dma((pieces,)),
            dma((pieces,)),
            dma((pieces,)),
            dma((pieces,)),
            dma((pieces, 2)),
            dma((pieces, 2)),
        ],
        compiler_params=pltpu.CompilerParams(
            collective_id=slots, has_side_effects=True, vmem_limit_bytes=62 * 2**20
        ),
        name="fused",
    )(
        plan,
        tokens.reshape(batches, length, depth),
        queries.reshape(batches, length, width),
        segment_ids,
        gain.reshape(1, depth),
        key_value_weight,
    )


def fused_shards(tokens, queries, segment_ids, gain, key_value_weight, plan):
    ranks = lax.axis_size("dp")
    batches = segment_ids.shape[0]
    most = batches * (ranks // 2)
    branches = [functools.partial(fused, slots) for slots in range(batches, most + 1)]
    source = np.arange(plan.shape[0]) // batches
    crossing = [
        jnp.sum(jnp.where(source < cut, plan >= cut * batches, False).astype(jnp.int32))
        for cut in range(2, ranks - 1)
    ]
    index = jnp.clip(functools.reduce(jnp.maximum, crossing, batches) - batches, 0, most - batches)
    return lax.switch(
        index, branches, plan, tokens, queries, segment_ids, gain, key_value_weight
    )


def solution(mesh):
    placed = (
        P(("dp", "fsdp"), "tensor"),
        P(("dp", "fsdp"), "tensor"),
        P(("dp", "fsdp"), None),
        P("tensor"),
        P("tensor", "fsdp"),
        P(),
    )
    small = mesh.shape["tensor"] == 2 and mesh.shape["fsdp"] == 4 and mesh.shape["dp"] <= 4
    return jax.shard_map(
        fused_shards if small else shards,
        mesh=mesh,
        in_specs=placed,
        out_specs=P(("dp", "fsdp"), "tensor"),
        check_vma=False,
    )
```

```python
import functools

import jax
import jax.numpy as jnp
import numpy as np
from jax import lax
from jax.experimental import pallas as pl
from jax.experimental.pallas import tpu as pltpu
from jax.sharding import PartitionSpec as P


HEAD_SIZE = 128


epsilon = 1e-05


def pack_query_kernel(send_ref, query_ref, out_ref):
    out_ref[...] = query_ref[...]


def pack_queries(send_index, queries, length):
    ranks = send_index.shape[0]
    width = queries.shape[1]
    return pl.pallas_call(
        pack_query_kernel,
        grid_spec=pltpu.PrefetchScalarGridSpec(
            num_scalar_prefetch=1,
            grid=(ranks,),
            in_specs=[pl.BlockSpec((length, width), lambda r, send: (send[r], 0))],
            out_specs=pl.BlockSpec((length, width), lambda r, send: (r, 0)),
        ),
        out_shape=jax.ShapeDtypeStruct((ranks * length, width), queries.dtype),
        name="pack_queries",
    )(send_index, queries)


def split_partial_kernel(part_ref, out_ref):
    key = part_ref[:, :HEAD_SIZE]
    high = key.astype(jnp.bfloat16)
    out_ref[:, :HEAD_SIZE] = high
    out_ref[:, HEAD_SIZE : 2 * HEAD_SIZE] = (key - high.astype(jnp.float32)).astype(jnp.bfloat16)
    out_ref[:, 2 * HEAD_SIZE :] = part_ref[:, HEAD_SIZE:].astype(jnp.bfloat16)


def split_partial(partial_value, ranks, spread):
    rows, width = partial_value.shape
    all_heads = width // (2 * HEAD_SIZE)
    heads = all_heads // spread
    height = rows // ranks
    return pl.pallas_call(
        split_partial_kernel,
        grid=(spread, ranks, heads),
        in_specs=[pl.BlockSpec((height, 2 * HEAD_SIZE), lambda b, f, h: (f, b * heads + h))],
        out_specs=pl.BlockSpec(
            (height, 3 * HEAD_SIZE), lambda b, f, h: ((b * ranks + f) * heads + h, 0)
        ),
        out_shape=jax.ShapeDtypeStruct((ranks * all_heads * height, 3 * HEAD_SIZE), jnp.bfloat16),
        name="split_partial",
    )(partial_value)


def pack_kv_kernel(sources, send_ref, slot_ref, *refs):
    *part_refs, document_ref, out_ref = refs
    part_heads = part_refs[0].shape[1]
    heads_kv = part_heads * len(part_refs) // sources
    for h in range(heads_kv):
        first = h // part_heads * sources
        key = value = 0.0
        for part_ref in part_refs[first : first + sources]:
            block = part_ref[0, h % part_heads, 0].astype(jnp.float32)
            key += block[:, :HEAD_SIZE] + block[:, HEAD_SIZE : 2 * HEAD_SIZE]
            value += block[:, 2 * HEAD_SIZE :]
        high = key.astype(jnp.bfloat16)
        low = (key - high.astype(jnp.float32)).astype(jnp.bfloat16)
        for place, part in enumerate((high, low, value.astype(jnp.bfloat16))):
            start = (place * heads_kv + h) * HEAD_SIZE
            out_ref[:, start : start + HEAD_SIZE] = part
    out_ref[:, 3 * heads_kv * HEAD_SIZE :] = document_ref[...]


def pack_kv(send_index, slot_index, parts, documents, sources, length):
    ranks = send_index.shape[0]
    count = slot_index.shape[0]
    rows = documents.shape[0]
    part_heads = parts.shape[0] // (count * rows)
    packed = (3 * part_heads * count // sources + 1) * HEAD_SIZE

    def arrived(w):
        return pl.BlockSpec(
            (1, part_heads, 1, length, 3 * HEAD_SIZE),
            lambda r, send, slot: (slot[w], 0, send[r], 0, 0),
        )

    view = parts.reshape(count, part_heads, rows // length, length, 3 * HEAD_SIZE)
    return pl.pallas_call(
        functools.partial(pack_kv_kernel, sources),
        grid_spec=pltpu.PrefetchScalarGridSpec(
            num_scalar_prefetch=2,
            grid=(ranks,),
            in_specs=[arrived(w) for w in range(count)]
            + [pl.BlockSpec((length, HEAD_SIZE), lambda r, send, slot: (send[r], 0))],
            out_specs=pl.BlockSpec((length, packed), lambda r, send, slot: (r, 0)),
        ),
        out_shape=jax.ShapeDtypeStruct((ranks * length, packed), jnp.bfloat16),
        name="pack_kv",
    )(send_index, slot_index, *[view] * count, documents)


def attend_kernel(
    head_group, keep_ref, query_ref, high_ref, low_ref, value_ref, document_ref, out_ref
):
    length = query_ref.shape[0]
    query = jnp.concatenate(
        [query_ref[:, g * HEAD_SIZE : (g + 1) * HEAD_SIZE] for g in range(head_group)], axis=0
    )
    across = (((1,), (1,)), ((), ()))
    scores = lax.dot_general(query, high_ref[...], across, preferred_element_type=jnp.float32)
    scores += lax.dot_general(query, low_ref[...], across, preferred_element_type=jnp.float32)
    scores = (scores * HEAD_SIZE ** (-0.5)).reshape(head_group, length, length)
    document = document_ref[...].astype(jnp.float32)
    rows = lax.broadcasted_iota(jnp.int32, (length, length), 0)
    columns = lax.broadcasted_iota(jnp.int32, (length, length), 1)
    allowed = (document == document.T) & (columns <= rows)
    scores = jnp.where(allowed[None], scores, -1e30)
    row_max = jnp.max(scores, axis=-1, keepdims=True)
    expo = jnp.exp(scores - row_max)
    weights = (expo / jnp.sum(expo, axis=-1, keepdims=True)).astype(jnp.bfloat16)
    mixed = jnp.dot(
        weights.reshape(head_group * length, length),
        value_ref[...],
        preferred_element_type=jnp.float32,
    ).astype(jnp.bfloat16)
    for g in range(head_group):
        out_ref[:, g * HEAD_SIZE : (g + 1) * HEAD_SIZE] = mixed[g * length : (g + 1) * length]


def attend(keep_index, queries, packed, length):
    batches = keep_index.shape[0]
    heads_kv = (packed.shape[1] // HEAD_SIZE - 1) // 3
    width = queries.shape[1]
    group_width = width // heads_kv

    def part(place):
        return pl.BlockSpec(
            (length, HEAD_SIZE), lambda s, h, keep: (keep[s], place * heads_kv + h)
        )

    return pl.pallas_call(
        functools.partial(attend_kernel, group_width // HEAD_SIZE),
        grid_spec=pltpu.PrefetchScalarGridSpec(
            num_scalar_prefetch=1,
            grid=(batches, heads_kv),
            in_specs=[
                pl.BlockSpec((length, group_width), lambda s, h, keep: (keep[s], h)),
                part(0),
                part(1),
                part(2),
                pl.BlockSpec((length, HEAD_SIZE), lambda s, h, keep: (keep[s], 3 * heads_kv)),
            ],
            out_specs=pl.BlockSpec((length, group_width), lambda s, h, keep: (s, h)),
        ),
        out_shape=jax.ShapeDtypeStruct((batches * length, width), jnp.bfloat16),
        name="attend",
    )(keep_index, queries, packed, packed, packed, packed)


def project(rows, gain, key_value_weight):
    all_rows = lax.all_gather(rows, "fsdp", axis=0, tiled=True)
    values = rows.astype(jnp.float32)
    own_stats = jnp.sum(values * values, axis=1)
    stats = lax.psum(own_stats, "tensor")
    full_width = rows.shape[1] * lax.axis_size("tensor")
    scale = lax.all_gather(lax.rsqrt(stats / full_width + epsilon), "fsdp", axis=0, tiled=True)
    normed = (all_rows.astype(jnp.float32) * scale[:, None] * gain).astype(jnp.bfloat16)
    partial_value = jnp.dot(normed, key_value_weight, preferred_element_type=jnp.float32)
    f_ranks, t_ranks = lax.axis_size("fsdp"), lax.axis_size("tensor")
    joined, spread = max(1, f_ranks // t_ranks), max(1, t_ranks // f_ranks)
    count = f_ranks * spread
    parts = split_partial(partial_value, f_ranks, spread)
    share = parts.shape[0] // count
    f, t = lax.axis_index("fsdp"), lax.axis_index("tensor")
    number = f % joined * t_ranks + t
    arrived = []
    for p in range(count):
        pairs = []
        for i in range(f_ranks):
            for j in range(t_ranks):
                block = (i % joined * t_ranks + j + p) % count
                target = i // joined * spread + block // f_ranks
                pairs.append((i * t_ranks + j, block % f_ranks * t_ranks + target))
        sent = lax.dynamic_slice_in_dim(parts, (number + p) % count * share, share)
        arrived.append(lax.ppermute(sent, ("fsdp", "tensor"), pairs))
    slot_index = (t % spread * f_ranks + f - jnp.arange(count, dtype=jnp.int32)) % count
    return jnp.concatenate(arrived), slot_index


def shards(tokens, queries, segment_ids, gain, key_value_weight, plan):
    rank_count = lax.axis_size("dp")
    own_rank = lax.axis_index("dp")
    batches, length = segment_ids.shape
    own_dest = lax.dynamic_slice_in_dim(plan, own_rank * batches, batches) // batches
    rank_range = jnp.arange(rank_count, dtype=jnp.int32)
    slot_range = jnp.arange(batches, dtype=jnp.int32)
    send_index = jnp.sum(
        jnp.where(own_dest[None, :] == rank_range[:, None], slot_range[None, :], 0), axis=1
    )
    position = jnp.arange(plan.shape[0], dtype=jnp.int32)
    own_slots = own_rank * batches + slot_range
    keep_index = jnp.sum(
        jnp.where(plan[None, :] == own_slots[:, None], position[None, :] // batches, 0), axis=1
    )
    parcels = pack_queries(send_index, queries, length)
    moved_queries = lax.all_to_all(parcels, "dp", split_axis=0, concat_axis=0, tiled=True)
    documents = jnp.broadcast_to(
        segment_ids.reshape(batches * length, 1).astype(jnp.bfloat16),
        (batches * length, HEAD_SIZE),
    )
    parts, slot_index = project(tokens, gain, key_value_weight)
    packed = pack_kv(
        send_index, slot_index, parts, documents, lax.axis_size("tensor"), length
    )
    packed, moved_queries = lax.optimization_barrier((packed, moved_queries))
    moved_kv = lax.all_to_all(packed, "dp", split_axis=0, concat_axis=0, tiled=True)
    return attend(keep_index, moved_queries, moved_kv, length)


def route(plan, ranks, batches, slots, me, step):
    order = list(range(ranks))[::step]
    held = [jnp.int32(-1)] * slots
    transit = [jnp.int32(0)] * slots
    second = [jnp.int32(0)] * slots
    arrived = [jnp.int32(-1)] * slots
    for rank in order:
        here = me == rank
        arrived = [jnp.where(here, held[j], arrived[j]) for j in range(slots)]
        own = [plan[rank * batches + s] for s in range(batches)]
        beyond = lambda place: (step * (place // batches - rank) > 0) & (place >= 0)
        waiting = [beyond(place).astype(jnp.int32) for place in own]
        following = []
        for j in range(slots):
            passes = beyond(held[j]).astype(jnp.int32)
            first_fits = (1 - passes) * waiting[0]
            second_fits = (1 - passes) * (1 - first_fits) * waiting[1]
            waiting = [waiting[0] - first_fits, waiting[1] - second_fits]
            transit[j] = jnp.where(here, passes, transit[j])
            second[j] = jnp.where(here, second_fits, second[j])
            following.append(
                jnp.where(
                    passes > 0,
                    held[j],
                    jnp.where(first_fits > 0, own[0], jnp.where(second_fits > 0, own[1], -1)),
                )
            )
        held = following
    return transit, second, arrived


def pack_parts(part):
    key = part[:, :HEAD_SIZE]
    high = key.astype(jnp.bfloat16)
    low = (key - high.astype(jnp.float32)).astype(jnp.bfloat16)
    return jnp.concatenate([high, low, part[:, HEAD_SIZE:].astype(jnp.bfloat16)], axis=1)


def unpack_parts(packed):
    wide = packed.astype(jnp.float32)
    key = wide[:, :HEAD_SIZE] + wide[:, HEAD_SIZE : 2 * HEAD_SIZE]
    return jnp.concatenate([key, wide[:, 2 * HEAD_SIZE :]], axis=1)


def fused_kernel(
    slots,
    plan_ref,
    tokens_ref,
    query_ref,
    document_ref,
    gain_ref,
    weight_ref,
    out_ref,
    own_rows,
    far_rows,
    weight,
    stats_own,
    stats_far,
    scale_own,
    scale_far,
    query_own,
    query_in,
    query_out,
    documents,
    own_parts,
    far_parts,
    parts_a,
    parts_b,
    kv_own,
    kv_out,
    *rest,
):
    pieces = parts_a.shape[0]
    kv_in = rest[:pieces]
    (
        load_rows,
        load_weight,
        load_query,
            rows_send,
        rows_recv,
        weight_send,
        weight_recv,
        stats_send,
        stats_recv,
        scale_send,
        scale_recv,
        query_send,
        query_recv,
        document_send,
        document_recv,
        own_send,
        far_send,
        a_recv,
        b_recv,
        kv_send,
        kv_recv,
    ) = rest[pieces:]
    ranks = lax.axis_size("dp")
    me, f, t = lax.axis_index("dp"), lax.axis_index("fsdp"), lax.axis_index("tensor")
    batches, length, depth = own_rows.shape
    heads = weight.shape[2] // HEAD_SIZE
    height = parts_a.shape[2]
    per_piece = pieces // heads
    tall = length // 4
    strips = batches * length // tall
    chunks, _, _, chunk_width = query_own.shape
    core = f % 2
    side = f // 2
    far = f + 2 - 4 * side
    pair = f + 1 - 2 * core
    other = 1 - t
    off = side != t
    away = side == t
    rounds = range(chunks)
    ahead = 2
    first = jnp.where(2 * me < ranks, 0, 1)
    second_way = 1 - first

    def remote(src, dst, send, recv, device):
        return pltpu.make_async_remote_copy(
            src_ref=src,
            dst_ref=dst,
            send_sem=send,
            recv_sem=recv,
            device_id=device,
            device_id_type=pl.DeviceIdType.MESH,
        )

    rows_local = pltpu.make_async_copy(tokens_ref, own_rows, load_rows)
    rows_local.start()
    query_local = []
    for c in rounds:
        query_local.append(
            pltpu.make_async_copy(
                query_ref.at[:, :, pl.ds(c * chunk_width, chunk_width)],
                query_own.at[c],
                load_query.at[c],
            )
        )
        query_local[c].start()
    weight_local = pltpu.make_async_copy(weight_ref, weight.at[core], load_weight)
    weight_local.start()

    barrier = pltpu.get_barrier_semaphore()
    partners = [(me, far, t), (me, pair, t), (me, f, other), (me, far, other)]
    partners += [((me + k) % ranks, f, t) for k in range(1, ranks)]
    for partner in partners:
        pl.semaphore_signal(
            barrier, inc=1, device_id=partner, device_id_type=pl.DeviceIdType.MESH
        )
    pl.semaphore_wait(barrier, len(partners))

    rows_moves = []
    for q in range(strips):
        part = (q % batches, pl.ds(q // batches * tall, tall))
        rows_moves.append(
            remote(
                tokens_ref.at[part],
                far_rows.at[part],
                rows_send.at[q],
                rows_recv.at[q],
                (me, far, t),
            )
        )

    for move in rows_moves[:ahead]:
        move.start()
    weight_move = remote(
        weight_ref, weight.at[core], weight_send, weight_recv, (me, pair, t)
    )
    weight_move.start()
    weight_arrives = remote(
        weight_ref, weight.at[1 - core], weight_send, weight_recv, (me, pair, t)
    )

    for s in range(batches):
        line = document_ref[s : s + 1, :].astype(jnp.float32)
        documents[me, s] = jnp.broadcast_to(line, (8, length))

    document_moves = [
        remote(
            documents.at[me],
            documents.at[me],
            document_send.at[k - 1],
            document_recv.at[k - 1],
            ((me + k) % ranks, f, t),
        )
        for k in range(1, ranks)
    ]
    document_arrivals = [
        remote(
            documents.at[(me + ranks - k) % ranks],
            documents.at[(me + ranks - k) % ranks],
            document_send.at[k - 1],
            document_recv.at[k - 1],
            ((me + k) % ranks, f, t),
        )
        for k in range(1, ranks)
    ]
    for move in document_moves:
        move.start()


    plan = [plan_ref[i] for i in range(ranks * batches)]
    routes = [route(plan, ranks, batches, slots, me, step) for step in (1, -1)]

    def has_in(way):
        return jnp.where(way == 0, me > 0, me < ranks - 1)

    def has_out(way):
        return jnp.where(way == 0, me < ranks - 1, me > 0)

    def chosen(name, j, way):
        return jnp.where(way == 0, routes[0][name][j], routes[1][name][j])

    def onward(way):
        return (me + 1 - 2 * way, f, t)

    def query_copy(way, c):
        return remote(
            query_out.at[c, way],
            query_in.at[c, way],
            query_send.at[c, way],
            query_recv.at[c, way],
            onward(way),
        )

    def query_step(way, c):
        @pl.when(has_out(way))
        def _():
            @pl.when(has_in(way))
            def _():
                query_copy(way, c).wait_recv()

            for j in range(slots):
                own = jnp.where(
                    chosen(1, j, way) > 0, query_own[c, 1], query_own[c, 0]
                )
                query_out[c, way, j] = jnp.where(
                    chosen(0, j, way) > 0, query_in[c, way, j], own
                )
            query_copy(way, c).start()

    for move in query_local:
        move.wait()
    middle = (me > 0) & (me < ranks - 1)
    ends = (me == 0) | (me == ranks - 1)

    @pl.when(ends)
    def _():
        @pl.loop(0, chunks)
        def _(c):
            query_step(first, c)

    def query_round(c):
        @pl.when(middle)
        def _():
            if c < chunks:
                query_step(first, c)
            if c:
                query_step(second_way, c - 1)

    rows_of = lax.broadcasted_iota(jnp.int32, (length, length), 0)
    columns_of = lax.broadcasted_iota(jnp.int32, (length, length), 1)
    diagonal = rows_of == columns_of
    block = 4 * HEAD_SIZE
    blocks = depth // block

    rows_local.wait()
    for s in range(batches):

        def squares(i, total, s=s):
            start = pl.multiple_of(i * block, block)
            values = own_rows[s, :, pl.ds(start, block)].astype(jnp.float32)
            values = values * values
            for g in range(block // HEAD_SIZE):
                total += values[:, g * HEAD_SIZE : (g + 1) * HEAD_SIZE]
            return total

        total = lax.fori_loop(
            0, blocks, squares, jnp.zeros((length, HEAD_SIZE), jnp.float32)
        )
        column = jnp.sum(total, axis=1, keepdims=True)
        line = jnp.sum(jnp.where(diagonal, column, 0.0), axis=0, keepdims=True)
        stats_own[s] = jnp.broadcast_to(line, (8, length))
    stats_move = remote(stats_own, stats_far, stats_send, stats_recv, (me, f, other))
    stats_move.start()
    stats_move.wait_recv()
    full_width = depth * lax.axis_size("tensor")
    scale_own[...] = lax.rsqrt((stats_own[...] + stats_far[...]) / full_width + epsilon)
    scale_move = remote(scale_own, scale_far, scale_send, scale_recv, (me, far, t))
    scale_move.start()
    for move in rows_moves[ahead:]:
        move.start()

    def normalize(rows, scale, s, top, count):
        line = jnp.broadcast_to(scale[s, 0:1, :], (length, length))
        column = jnp.sum(jnp.where(diagonal, line, 0.0), axis=1, keepdims=True)
        column = column[top : top + count]

        @pl.loop(0, blocks)
        def _(i):
            start = pl.multiple_of(i * block, block)
            values = rows[s, top : top + count, pl.ds(start, block)].astype(jnp.float32)
            values = values * column * gain_ref[:, pl.ds(start, block)]
            rows[s, top : top + count, pl.ds(start, block)] = values.astype(jnp.bfloat16)

    for s in range(batches):
        normalize(own_rows, scale_own, s, 0, length)

    def multiply(rows, h):
        count = rows.shape[1]
        half = heads // 2
        start = pl.multiple_of((h % half) * 2 * HEAD_SIZE, 2 * HEAD_SIZE)
        part = jnp.dot(
            rows.reshape(batches * count, depth),
            weight[h // half, :, pl.ds(start, 2 * HEAD_SIZE)],
            preferred_element_type=jnp.float32,
        )
        return pack_parts(part).reshape(batches, count, 3 * HEAD_SIZE)

    def own_copy(i):
        return remote(
            own_parts.at[i], parts_b.at[i], own_send.at[i], b_recv.at[i], (me, f, other)
        )

    def far_copy_a(i):
        return remote(
            far_parts.at[i], parts_a.at[i], far_send.at[i], a_recv.at[i], (me, far, t)
        )

    def far_copy_b(i):
        return remote(
            far_parts.at[i], parts_b.at[i], far_send.at[i], b_recv.at[i], (me, far, other)
        )

    def own_head(h):
        packed = multiply(own_rows[...], h)
        for j in range(per_piece):
            i = j * heads + h
            piece = packed[:, j * height : (j + 1) * height]

            @pl.when(off)
            def _():
                own_parts[i] = piece
                own_copy(i).start()

            @pl.when(away)
            def _():
                parts_a[i] = piece

    def send_far(i):
        top = i // heads * height
        far_parts[i] = multiply(far_rows[:, top : top + height], i % heads)

        @pl.when(off)
        def _():
            far_copy_b(i).start()

        @pl.when(away)
        def _():
            far_copy_a(i).start()

    def take_rows(q):
        rows_moves[q].wait_recv()
        if q == 0:
            scale_move.wait_recv()
        normalize(far_rows, scale_far, q % batches, q // batches * tall, tall)

    taken = early = 0
    later = list(range(chunks + 1))
    while taken < strips:
        c = later.pop(0)
        query_round(c)
        paced = (c + 1) * slots * length * chunk_width // (tall * depth)
        if c == 0:
            weight_local.wait()
            weight_arrives.wait_recv()
        if c < 2:
            pl.loop(c * heads // 2, (c + 1) * heads // 2)(own_head)
        upto = paced
        if (c + 2) * slots * length * chunk_width >= strips * tall * depth:
            upto = strips
        while taken < upto:
            take_rows(taken)
            taken += 1
        if early < heads and taken * tall >= batches * height:
            send_far(early)
            early += 1

    def kv_copy(way, h):
        return remote(
            kv_out.at[h, way],
            kv_in[h].at[way],
            kv_send.at[h, way],
            kv_recv.at[h, way],
            onward(way),
        )

    def kv_step(way, h):
        @pl.when(has_out(way))
        def _():
            @pl.when(has_in(way))
            def _():
                kv_copy(way, h).wait_recv()

            for j in range(slots):
                own = jnp.where(chosen(1, j, way) > 0, kv_own[h, 1], kv_own[h, 0])
                kv_out[h, way, j] = jnp.where(
                    chosen(0, j, way) > 0, kv_in[h][way, j], own
                )
            kv_copy(way, h).start()

    def join(h):
        @pl.when(off)
        def _():
            far_copy_a(h).wait_recv()

        far_copy_b(h).wait_recv()
        for s in range(batches):
            kv_own[h, s] = pack_parts(
                unpack_parts(parts_a[h, s]) + unpack_parts(parts_b[h, s])
            )

    per_head = chunks // heads
    group = per_head * chunk_width // HEAD_SIZE
    across = (((1,), (1,)), ((), ()))

    def place_of(s):
        want = me * batches + s
        own_at = jnp.int32(-1)
        for b in range(batches):
            for rank in range(ranks):
                hit = (me == rank) & (plan[rank * batches + b] == want)
                own_at = jnp.where(hit, b, own_at)
        in_at = []
        for way in range(2):
            at = jnp.int32(-1)
            for j in range(slots):
                at = jnp.where(routes[way][2][j] == want, j, at)
            in_at.append(at)
        source = jnp.int32(0)
        for b in range(ranks * batches):
            source = jnp.where(plan[b] == want, b, source)
        return own_at, in_at[0], in_at[1], source

    def pick(own, coming, places):
        own_at, right_at, left_at, _ = places
        value = jnp.where(
            right_at >= 0, coming(0, jnp.maximum(right_at, 0)), own(jnp.maximum(own_at, 0))
        )
        return jnp.where(left_at >= 0, coming(1, jnp.maximum(left_at, 0)), value)

    spots = [place_of(s) for s in range(batches)]

    def settle(copy, index):
        for way in range(2):

            @pl.when(has_in(way) & jnp.logical_not(has_out(way)))
            def _():
                copy(way, index).wait_recv()

    def attend_head(h):
        for i in range(h, pieces, heads):
            settle(kv_copy, i)

        @pl.loop(0, batches)
        def _(s):
            places = [jnp.where(s == 0, a, b) for a, b in zip(*spots)]
            tiles = []
            for c in range(h * per_head, (h + 1) * per_head):
                wide = pick(
                    lambda at: query_own[c, at], lambda way, at: query_in[c, way, at], places
                )
                for g in range(chunk_width // HEAD_SIZE):
                    tiles.append(wide[:, g * HEAD_SIZE : (g + 1) * HEAD_SIZE])
            query = jnp.concatenate(tiles, axis=0)
            kv = jnp.concatenate(
                [
                    pick(lambda at: kv_own[i, at], lambda way, at: kv_in[i][way, at], places)
                    for i in range(h, pieces, heads)
                ],
                axis=0,
            )
            high, low, value = (
                kv[:, i * HEAD_SIZE : (i + 1) * HEAD_SIZE] for i in range(3)
            )
            line = documents[places[3] // batches, places[3] % batches]
            line = jnp.broadcast_to(line[0:1, :], (length, length))
            scores = lax.dot_general(query, high, across, preferred_element_type=jnp.float32)
            scores += lax.dot_general(query, low, across, preferred_element_type=jnp.float32)
            scores = (scores * HEAD_SIZE ** (-0.5)).reshape(group, length, length)
            allowed = (line == line.T) & (columns_of <= rows_of)
            scores = jnp.where(allowed[None], scores, -1e30)
            row_max = jnp.max(scores, axis=-1, keepdims=True)
            expo = jnp.exp(scores - row_max)
            weights = (expo / jnp.sum(expo, axis=-1, keepdims=True)).astype(jnp.bfloat16)
            result = jnp.dot(
                weights.reshape(group * length, length),
                value,
                preferred_element_type=jnp.float32,
            ).astype(jnp.bfloat16)
            top = pl.multiple_of(s * length, length)
            for g in range(group):
                start = (h * group + g) * HEAD_SIZE
                out_ref[pl.ds(top, length), start : start + HEAD_SIZE] = result[
                    g * length : (g + 1) * length
                ]

    def kv_round(i):
        join(i)
        kv_step(first, i)
        if i == 1:
            query_round(later.pop(0))
        if i >= 2:
            kv_step(second_way, i - 2)

    rounds_done = 0
    for i in range(early, pieces):
        send_far(i)
        if i >= heads and len(later) > 1:
            query_round(later.pop(0))
        elif i > heads and len(later) <= 1:
            kv_round(rounds_done)
            rounds_done += 1
    while len(later) > 1:
        query_round(later.pop(0))
    for i in range(rounds_done, pieces):
        kv_round(i)
    for i in range(pieces - 2, pieces):
        kv_step(second_way, i)
    for c in rounds:
        settle(query_copy, c)
    for move in document_arrivals:
        move.wait_recv()
    for h in range(heads):
        attend_head(h)

    for move in rows_moves + [weight_move, stats_move, scale_move] + document_moves:
        move.wait_send()
    for way in range(2):

        @pl.when(has_out(way))
        def _():
            for c in rounds:
                query_copy(way, c).wait_send()
            for i in range(pieces):
                kv_copy(way, i).wait_send()

    for i in range(pieces):

        @pl.when(off)
        def _():
            own_copy(i).wait_send()

        far_copy_a(i).wait_send()


def fused(slots, plan, tokens, queries, segment_ids, gain, key_value_weight):
    ranks = lax.axis_size("dp")
    batches, length = segment_ids.shape
    rows, depth = tokens.shape
    width = queries.shape[1]
    heads = 2 * key_value_weight.shape[1] // (2 * HEAD_SIZE)
    chunks = 4 * heads
    chunk_width = width // chunks
    pieces = 2 * heads
    packed = (length // 2, 3 * HEAD_SIZE)
    bf16, f32 = jnp.bfloat16, jnp.float32
    limit = (5 + slots) * 6 * 2**20
    dma = pltpu.SemaphoreType.DMA
    anywhere = pl.BlockSpec(memory_space=pl.ANY)
    return pl.pallas_call(
        functools.partial(fused_kernel, slots),
        out_shape=jax.ShapeDtypeStruct((rows, width), bf16),
        in_specs=[
            pl.BlockSpec(memory_space=pltpu.SMEM),
            anywhere,
            anywhere,
            pl.BlockSpec(memory_space=pltpu.VMEM),
            pl.BlockSpec(memory_space=pltpu.VMEM),
            anywhere,
        ],
        out_specs=pl.BlockSpec(memory_space=pltpu.VMEM),
        scratch_shapes=[
            pltpu.VMEM((batches, length, depth), bf16),
            pltpu.VMEM((batches, length, depth), bf16),
            pltpu.VMEM((2, depth, key_value_weight.shape[1]), bf16),
            pltpu.VMEM((batches, 8, length), f32),
            pltpu.VMEM((batches, 8, length), f32),
            pltpu.VMEM((batches, 8, length), f32),
            pltpu.VMEM((batches, 8, length), f32),
            pltpu.VMEM((chunks, batches, length, chunk_width), bf16),
            pltpu.VMEM((chunks, 2, slots, length, chunk_width), bf16),
            pltpu.VMEM((chunks, 2, slots, length, chunk_width), bf16),
            pltpu.VMEM((ranks, batches, 8, length), f32),
            pltpu.VMEM((pieces, batches, *packed), bf16),
            pltpu.VMEM((pieces, batches, *packed), bf16),
            pltpu.VMEM((pieces, batches, *packed), bf16),
            pltpu.VMEM((pieces, batches, *packed), bf16),
            pltpu.VMEM((pieces, batches, *packed), bf16),
            pltpu.VMEM((pieces, 2, slots, *packed), bf16),
        ]
        + [pltpu.VMEM((2, slots, *packed), bf16)] * pieces
        + [
            dma,
            dma,
            dma((chunks,)),
            dma((4 * batches,)),
            dma((4 * batches,)),
            dma,
            dma,
            dma,
            dma,
            dma,
            dma,
            dma((chunks, 2)),
            dma((chunks, 2)),
            dma((ranks - 1,)),
            dma((ranks - 1,)),
            dma((pieces,)),
            dma((pieces,)),
            dma((pieces,)),
            dma((pieces,)),
            dma((pieces, 2)),
            dma((pieces, 2)),
        ],
        compiler_params=pltpu.CompilerParams(
            collective_id=slots, has_side_effects=True, vmem_limit_bytes=limit
        ),
        name="fused",
    )(
        plan,
        tokens.reshape(batches, length, depth),
        queries.reshape(batches, length, width),
        segment_ids,
        gain.reshape(1, depth),
        key_value_weight,
    )


def fused_shards(tokens, queries, segment_ids, gain, key_value_weight, plan):
    ranks = lax.axis_size("dp")
    batches = segment_ids.shape[0]
    most = batches * (ranks // 2)
    branches = [functools.partial(fused, slots) for slots in range(batches, most + 1)]
    source = np.arange(plan.shape[0]) // batches
    crossing = [
        jnp.sum(jnp.where(source < cut, plan >= cut * batches, False).astype(jnp.int32))
        for cut in range(2, ranks - 1)
    ]
    index = jnp.clip(functools.reduce(jnp.maximum, crossing, batches) - batches, 0, most - batches)
    return lax.switch(
        index, branches, plan, tokens, queries, segment_ids, gain, key_value_weight
    )


def solution(mesh):
    placed = (
        P(("dp", "fsdp"), "tensor"),
        P(("dp", "fsdp"), "tensor"),
        P(("dp", "fsdp"), None),
        P("tensor"),
        P("tensor", "fsdp"),
        P(),
    )
    small = mesh.shape["tensor"] == 2 and mesh.shape["fsdp"] == 4 and mesh.shape["dp"] <= 4
    return jax.shard_map(
        fused_shards if small else shards,
        mesh=mesh,
        in_specs=placed,
        out_specs=P(("dp", "fsdp"), "tensor"),
        check_vma=False,
    )
```

```python
import functools

import jax
import jax.numpy as jnp
import numpy as np
from jax import lax
from jax.experimental import pallas as pl
from jax.experimental.pallas import tpu as pltpu
from jax.sharding import PartitionSpec as P


HEAD_SIZE = 128


epsilon = 1e-05


def pack_query_kernel(send_ref, query_ref, out_ref):
    out_ref[...] = query_ref[...]


def pack_queries(send_index, queries, length):
    ranks = send_index.shape[0]
    width = queries.shape[1]
    return pl.pallas_call(
        pack_query_kernel,
        grid_spec=pltpu.PrefetchScalarGridSpec(
            num_scalar_prefetch=1,
            grid=(ranks,),
            in_specs=[pl.BlockSpec((length, width), lambda r, send: (send[r], 0))],
            out_specs=pl.BlockSpec((length, width), lambda r, send: (r, 0)),
        ),
        out_shape=jax.ShapeDtypeStruct((ranks * length, width), queries.dtype),
        name="pack_queries",
    )(send_index, queries)


def split_partial_kernel(part_ref, out_ref):
    key = part_ref[:, :HEAD_SIZE]
    high = key.astype(jnp.bfloat16)
    out_ref[:, :HEAD_SIZE] = high
    out_ref[:, HEAD_SIZE : 2 * HEAD_SIZE] = (key - high.astype(jnp.float32)).astype(jnp.bfloat16)
    out_ref[:, 2 * HEAD_SIZE :] = part_ref[:, HEAD_SIZE:].astype(jnp.bfloat16)


def split_partial(partial_value, ranks, spread):
    rows, width = partial_value.shape
    all_heads = width // (2 * HEAD_SIZE)
    heads = all_heads // spread
    height = rows // ranks
    return pl.pallas_call(
        split_partial_kernel,
        grid=(spread, ranks, heads),
        in_specs=[pl.BlockSpec((height, 2 * HEAD_SIZE), lambda b, f, h: (f, b * heads + h))],
        out_specs=pl.BlockSpec(
            (height, 3 * HEAD_SIZE), lambda b, f, h: ((b * ranks + f) * heads + h, 0)
        ),
        out_shape=jax.ShapeDtypeStruct((ranks * all_heads * height, 3 * HEAD_SIZE), jnp.bfloat16),
        name="split_partial",
    )(partial_value)


def pack_kv_kernel(sources, send_ref, slot_ref, *refs):
    *part_refs, document_ref, out_ref = refs
    part_heads = part_refs[0].shape[1]
    heads_kv = part_heads * len(part_refs) // sources
    for h in range(heads_kv):
        first = h // part_heads * sources
        key = value = 0.0
        for part_ref in part_refs[first : first + sources]:
            block = part_ref[0, h % part_heads, 0].astype(jnp.float32)
            key += block[:, :HEAD_SIZE] + block[:, HEAD_SIZE : 2 * HEAD_SIZE]
            value += block[:, 2 * HEAD_SIZE :]
        high = key.astype(jnp.bfloat16)
        low = (key - high.astype(jnp.float32)).astype(jnp.bfloat16)
        for place, part in enumerate((high, low, value.astype(jnp.bfloat16))):
            start = (place * heads_kv + h) * HEAD_SIZE
            out_ref[:, start : start + HEAD_SIZE] = part
    out_ref[:, 3 * heads_kv * HEAD_SIZE :] = document_ref[...]


def pack_kv(send_index, slot_index, parts, documents, sources, length):
    ranks = send_index.shape[0]
    count = slot_index.shape[0]
    rows = documents.shape[0]
    part_heads = parts.shape[0] // (count * rows)
    packed = (3 * part_heads * count // sources + 1) * HEAD_SIZE

    def arrived(w):
        return pl.BlockSpec(
            (1, part_heads, 1, length, 3 * HEAD_SIZE),
            lambda r, send, slot: (slot[w], 0, send[r], 0, 0),
        )

    view = parts.reshape(count, part_heads, rows // length, length, 3 * HEAD_SIZE)
    return pl.pallas_call(
        functools.partial(pack_kv_kernel, sources),
        grid_spec=pltpu.PrefetchScalarGridSpec(
            num_scalar_prefetch=2,
            grid=(ranks,),
            in_specs=[arrived(w) for w in range(count)]
            + [pl.BlockSpec((length, HEAD_SIZE), lambda r, send, slot: (send[r], 0))],
            out_specs=pl.BlockSpec((length, packed), lambda r, send, slot: (r, 0)),
        ),
        out_shape=jax.ShapeDtypeStruct((ranks * length, packed), jnp.bfloat16),
        name="pack_kv",
    )(send_index, slot_index, *[view] * count, documents)


def attend_kernel(
    head_group, keep_ref, query_ref, high_ref, low_ref, value_ref, document_ref, out_ref
):
    length = query_ref.shape[0]
    query = jnp.concatenate(
        [query_ref[:, g * HEAD_SIZE : (g + 1) * HEAD_SIZE] for g in range(head_group)], axis=0
    )
    across = (((1,), (1,)), ((), ()))
    scores = lax.dot_general(query, high_ref[...], across, preferred_element_type=jnp.float32)
    scores += lax.dot_general(query, low_ref[...], across, preferred_element_type=jnp.float32)
    scores = (scores * HEAD_SIZE ** (-0.5)).reshape(head_group, length, length)
    document = document_ref[...].astype(jnp.float32)
    rows = lax.broadcasted_iota(jnp.int32, (length, length), 0)
    columns = lax.broadcasted_iota(jnp.int32, (length, length), 1)
    allowed = (document == document.T) & (columns <= rows)
    scores = jnp.where(allowed[None], scores, -1e30)
    row_max = jnp.max(scores, axis=-1, keepdims=True)
    expo = jnp.exp(scores - row_max)
    weights = (expo / jnp.sum(expo, axis=-1, keepdims=True)).astype(jnp.bfloat16)
    mixed = jnp.dot(
        weights.reshape(head_group * length, length),
        value_ref[...],
        preferred_element_type=jnp.float32,
    ).astype(jnp.bfloat16)
    for g in range(head_group):
        out_ref[:, g * HEAD_SIZE : (g + 1) * HEAD_SIZE] = mixed[g * length : (g + 1) * length]


def attend(keep_index, queries, packed, length):
    batches = keep_index.shape[0]
    heads_kv = (packed.shape[1] // HEAD_SIZE - 1) // 3
    width = queries.shape[1]
    group_width = width // heads_kv

    def part(place):
        return pl.BlockSpec(
            (length, HEAD_SIZE), lambda s, h, keep: (keep[s], place * heads_kv + h)
        )

    return pl.pallas_call(
        functools.partial(attend_kernel, group_width // HEAD_SIZE),
        grid_spec=pltpu.PrefetchScalarGridSpec(
            num_scalar_prefetch=1,
            grid=(batches, heads_kv),
            in_specs=[
                pl.BlockSpec((length, group_width), lambda s, h, keep: (keep[s], h)),
                part(0),
                part(1),
                part(2),
                pl.BlockSpec((length, HEAD_SIZE), lambda s, h, keep: (keep[s], 3 * heads_kv)),
            ],
            out_specs=pl.BlockSpec((length, group_width), lambda s, h, keep: (s, h)),
        ),
        out_shape=jax.ShapeDtypeStruct((batches * length, width), jnp.bfloat16),
        name="attend",
    )(keep_index, queries, packed, packed, packed, packed)


def project(rows, gain, key_value_weight):
    all_rows = lax.all_gather(rows, "fsdp", axis=0, tiled=True)
    values = rows.astype(jnp.float32)
    own_stats = jnp.sum(values * values, axis=1)
    stats = lax.psum(own_stats, "tensor")
    full_width = rows.shape[1] * lax.axis_size("tensor")
    scale = lax.all_gather(lax.rsqrt(stats / full_width + epsilon), "fsdp", axis=0, tiled=True)
    normed = (all_rows.astype(jnp.float32) * scale[:, None] * gain).astype(jnp.bfloat16)
    partial_value = jnp.dot(normed, key_value_weight, preferred_element_type=jnp.float32)
    f_ranks, t_ranks = lax.axis_size("fsdp"), lax.axis_size("tensor")
    joined, spread = max(1, f_ranks // t_ranks), max(1, t_ranks // f_ranks)
    count = f_ranks * spread
    parts = split_partial(partial_value, f_ranks, spread)
    share = parts.shape[0] // count
    f, t = lax.axis_index("fsdp"), lax.axis_index("tensor")
    number = f % joined * t_ranks + t
    arrived = []
    for p in range(count):
        pairs = []
        for i in range(f_ranks):
            for j in range(t_ranks):
                block = (i % joined * t_ranks + j + p) % count
                target = i // joined * spread + block // f_ranks
                pairs.append((i * t_ranks + j, block % f_ranks * t_ranks + target))
        sent = lax.dynamic_slice_in_dim(parts, (number + p) % count * share, share)
        arrived.append(lax.ppermute(sent, ("fsdp", "tensor"), pairs))
    slot_index = (t % spread * f_ranks + f - jnp.arange(count, dtype=jnp.int32)) % count
    return jnp.concatenate(arrived), slot_index


def shards(tokens, queries, segment_ids, gain, key_value_weight, plan):
    rank_count = lax.axis_size("dp")
    own_rank = lax.axis_index("dp")
    batches, length = segment_ids.shape
    own_dest = lax.dynamic_slice_in_dim(plan, own_rank * batches, batches) // batches
    rank_range = jnp.arange(rank_count, dtype=jnp.int32)
    slot_range = jnp.arange(batches, dtype=jnp.int32)
    send_index = jnp.sum(
        jnp.where(own_dest[None, :] == rank_range[:, None], slot_range[None, :], 0), axis=1
    )
    position = jnp.arange(plan.shape[0], dtype=jnp.int32)
    own_slots = own_rank * batches + slot_range
    keep_index = jnp.sum(
        jnp.where(plan[None, :] == own_slots[:, None], position[None, :] // batches, 0), axis=1
    )
    parcels = pack_queries(send_index, queries, length)
    moved_queries = lax.all_to_all(parcels, "dp", split_axis=0, concat_axis=0, tiled=True)
    documents = jnp.broadcast_to(
        segment_ids.reshape(batches * length, 1).astype(jnp.bfloat16),
        (batches * length, HEAD_SIZE),
    )
    parts, slot_index = project(tokens, gain, key_value_weight)
    packed = pack_kv(
        send_index, slot_index, parts, documents, lax.axis_size("tensor"), length
    )
    packed, moved_queries = lax.optimization_barrier((packed, moved_queries))
    moved_kv = lax.all_to_all(packed, "dp", split_axis=0, concat_axis=0, tiled=True)
    return attend(keep_index, moved_queries, moved_kv, length)


def route(plan, ranks, batches, slots, me, step):
    order = list(range(ranks))[::step]
    held = [jnp.int32(-1)] * slots
    transit = [jnp.int32(0)] * slots
    second = [jnp.int32(0)] * slots
    arrived = [jnp.int32(-1)] * slots
    for rank in order:
        here = me == rank
        arrived = [jnp.where(here, held[j], arrived[j]) for j in range(slots)]
        own = [plan[rank * batches + s] for s in range(batches)]
        beyond = lambda place: (step * (place // batches - rank) > 0) & (place >= 0)
        waiting = [beyond(place).astype(jnp.int32) for place in own]
        following = []
        for j in range(slots):
            passes = beyond(held[j]).astype(jnp.int32)
            first_fits = (1 - passes) * waiting[0]
            second_fits = (1 - passes) * (1 - first_fits) * waiting[1]
            waiting = [waiting[0] - first_fits, waiting[1] - second_fits]
            transit[j] = jnp.where(here, passes, transit[j])
            second[j] = jnp.where(here, second_fits, second[j])
            following.append(
                jnp.where(
                    passes > 0,
                    held[j],
                    jnp.where(first_fits > 0, own[0], jnp.where(second_fits > 0, own[1], -1)),
                )
            )
        held = following
    return transit, second, arrived


def pack_parts(part):
    key = part[:, :HEAD_SIZE]
    high = key.astype(jnp.bfloat16)
    low = (key - high.astype(jnp.float32)).astype(jnp.bfloat16)
    return jnp.concatenate([high, low, part[:, HEAD_SIZE:].astype(jnp.bfloat16)], axis=1)


def unpack_parts(packed):
    wide = packed.astype(jnp.float32)
    key = wide[:, :HEAD_SIZE] + wide[:, HEAD_SIZE : 2 * HEAD_SIZE]
    return jnp.concatenate([key, wide[:, 2 * HEAD_SIZE :]], axis=1)


def fused_kernel(
    slots,
    plan_ref,
    tokens_ref,
    query_ref,
    document_ref,
    gain_ref,
    weight_ref,
    out_ref,
    own_rows,
    far_rows,
    weight,
    stats_own,
    stats_far,
    scale_own,
    scale_far,
    query_own,
    query_in,
    query_out,
    documents,
    own_parts,
    far_parts,
    parts_a,
    parts_b,
    kv_own,
    kv_out,
    *rest,
):
    pieces = parts_a.shape[0]
    kv_in = rest[:pieces]
    (
        load_rows,
        load_weight,
        load_query,
            rows_send,
        rows_recv,
        weight_send,
        weight_recv,
        stats_send,
        stats_recv,
        scale_send,
        scale_recv,
        query_send,
        query_recv,
        document_send,
        document_recv,
        own_send,
        far_send,
        a_recv,
        b_recv,
        kv_send,
        kv_recv,
    ) = rest[pieces:]
    ranks = lax.axis_size("dp")
    me, f, t = lax.axis_index("dp"), lax.axis_index("fsdp"), lax.axis_index("tensor")
    batches, length, depth = own_rows.shape
    heads = weight.shape[2] // HEAD_SIZE
    height = parts_a.shape[2]
    per_piece = pieces // heads
    tall = length // 4
    strips = batches * length // tall
    chunks, _, _, chunk_width = query_own.shape
    core = f % 2
    side = f // 2
    far = f + 2 - 4 * side
    pair = f + 1 - 2 * core
    other = 1 - t
    off = side != t
    away = side == t
    rounds = range(chunks)
    ahead = 1
    first = jnp.where(2 * me < ranks, 0, 1)
    second_way = 1 - first

    def remote(src, dst, send, recv, device):
        return pltpu.make_async_remote_copy(
            src_ref=src,
            dst_ref=dst,
            send_sem=send,
            recv_sem=recv,
            device_id=device,
            device_id_type=pl.DeviceIdType.MESH,
        )

    rows_local = pltpu.make_async_copy(tokens_ref, own_rows, load_rows)
    rows_local.start()
    query_local = []
    for c in rounds:
        query_local.append(
            pltpu.make_async_copy(
                query_ref.at[:, :, pl.ds(c * chunk_width, chunk_width)],
                query_own.at[c],
                load_query.at[c],
            )
        )
        query_local[c].start()
    weight_local = pltpu.make_async_copy(weight_ref, weight.at[core], load_weight)
    weight_local.start()

    barrier = pltpu.get_barrier_semaphore()
    partners = [(me, far, t), (me, pair, t), (me, f, other), (me, far, other)]
    partners += [((me + k) % ranks, f, t) for k in range(1, ranks)]
    for partner in partners:
        pl.semaphore_signal(
            barrier, inc=1, device_id=partner, device_id_type=pl.DeviceIdType.MESH
        )
    pl.semaphore_wait(barrier, len(partners))

    rows_moves = []
    for q in range(strips):
        part = (q % batches, pl.ds(q // batches * tall, tall))
        rows_moves.append(
            remote(
                tokens_ref.at[part],
                far_rows.at[part],
                rows_send.at[q],
                rows_recv.at[q],
                (me, far, t),
            )
        )

    for move in rows_moves[:ahead]:
        move.start()
    weight_move = remote(
        weight_ref, weight.at[core], weight_send, weight_recv, (me, pair, t)
    )
    weight_move.start()
    weight_arrives = remote(
        weight_ref, weight.at[1 - core], weight_send, weight_recv, (me, pair, t)
    )

    for s in range(batches):
        line = document_ref[s : s + 1, :].astype(jnp.float32)
        documents[me, s] = jnp.broadcast_to(line, (8, length))

    document_moves = [
        remote(
            documents.at[me],
            documents.at[me],
            document_send.at[k - 1],
            document_recv.at[k - 1],
            ((me + k) % ranks, f, t),
        )
        for k in range(1, ranks)
    ]
    document_arrivals = [
        remote(
            documents.at[(me + ranks - k) % ranks],
            documents.at[(me + ranks - k) % ranks],
            document_send.at[k - 1],
            document_recv.at[k - 1],
            ((me + k) % ranks, f, t),
        )
        for k in range(1, ranks)
    ]
    for move in document_moves:
        move.start()


    plan = [plan_ref[i] for i in range(ranks * batches)]
    routes = [route(plan, ranks, batches, slots, me, step) for step in (1, -1)]

    def has_in(way):
        return jnp.where(way == 0, me > 0, me < ranks - 1)

    def has_out(way):
        return jnp.where(way == 0, me < ranks - 1, me > 0)

    def chosen(name, j, way):
        return jnp.where(way == 0, routes[0][name][j], routes[1][name][j])

    def onward(way):
        return (me + 1 - 2 * way, f, t)

    def query_copy(way, c):
        return remote(
            query_out.at[c, way],
            query_in.at[c, way],
            query_send.at[c, way],
            query_recv.at[c, way],
            onward(way),
        )

    def query_step(way, c):
        @pl.when(has_out(way))
        def _():
            @pl.when(has_in(way))
            def _():
                query_copy(way, c).wait_recv()

            for j in range(slots):
                own = jnp.where(
                    chosen(1, j, way) > 0, query_own[c, 1], query_own[c, 0]
                )
                query_out[c, way, j] = jnp.where(
                    chosen(0, j, way) > 0, query_in[c, way, j], own
                )
            query_copy(way, c).start()

    for move in query_local:
        move.wait()
    middle = (me > 0) & (me < ranks - 1)
    ends = (me == 0) | (me == ranks - 1)

    @pl.when(ends)
    def _():
        @pl.loop(0, chunks)
        def _(c):
            query_step(first, c)

    def query_round(c):
        @pl.when(middle)
        def _():
            if c < chunks:
                query_step(first, c)
            if c:
                query_step(second_way, c - 1)

    rows_of = lax.broadcasted_iota(jnp.int32, (length, length), 0)
    columns_of = lax.broadcasted_iota(jnp.int32, (length, length), 1)
    diagonal = rows_of == columns_of
    block = 4 * HEAD_SIZE
    blocks = depth // block

    rows_local.wait()
    for s in range(batches):

        def squares(i, total, s=s):
            start = pl.multiple_of(i * block, block)
            values = own_rows[s, :, pl.ds(start, block)].astype(jnp.float32)
            values = values * values
            for g in range(block // HEAD_SIZE):
                total += values[:, g * HEAD_SIZE : (g + 1) * HEAD_SIZE]
            return total

        total = lax.fori_loop(
            0, blocks, squares, jnp.zeros((length, HEAD_SIZE), jnp.float32)
        )
        column = jnp.sum(total, axis=1, keepdims=True)
        line = jnp.sum(jnp.where(diagonal, column, 0.0), axis=0, keepdims=True)
        stats_own[s] = jnp.broadcast_to(line, (8, length))
    stats_move = remote(stats_own, stats_far, stats_send, stats_recv, (me, f, other))
    stats_move.start()
    stats_move.wait_recv()
    full_width = depth * lax.axis_size("tensor")
    scale_own[...] = lax.rsqrt((stats_own[...] + stats_far[...]) / full_width + epsilon)
    scale_move = remote(scale_own, scale_far, scale_send, scale_recv, (me, far, t))
    scale_move.start()
    for move in rows_moves[ahead:]:
        move.start()

    def normalize(rows, scale, s, top, count):
        line = jnp.broadcast_to(scale[s, 0:1, :], (length, length))
        column = jnp.sum(jnp.where(diagonal, line, 0.0), axis=1, keepdims=True)
        column = column[top : top + count]

        @pl.loop(0, blocks)
        def _(i):
            start = pl.multiple_of(i * block, block)
            values = rows[s, top : top + count, pl.ds(start, block)].astype(jnp.float32)
            values = values * column * gain_ref[:, pl.ds(start, block)]
            rows[s, top : top + count, pl.ds(start, block)] = values.astype(jnp.bfloat16)

    for s in range(batches):
        normalize(own_rows, scale_own, s, 0, length)

    def multiply(rows, h):
        count = rows.shape[1]
        half = heads // 2
        start = pl.multiple_of((h % half) * 2 * HEAD_SIZE, 2 * HEAD_SIZE)
        part = jnp.dot(
            rows.reshape(batches * count, depth),
            weight[h // half, :, pl.ds(start, 2 * HEAD_SIZE)],
            preferred_element_type=jnp.float32,
        )
        return pack_parts(part).reshape(batches, count, 3 * HEAD_SIZE)

    def own_copy(i):
        return remote(
            own_parts.at[i], parts_b.at[i], own_send.at[i], b_recv.at[i], (me, f, other)
        )

    def far_copy_a(i):
        return remote(
            far_parts.at[i], parts_a.at[i], far_send.at[i], a_recv.at[i], (me, far, t)
        )

    def far_copy_b(i):
        return remote(
            far_parts.at[i], parts_b.at[i], far_send.at[i], b_recv.at[i], (me, far, other)
        )

    def own_head(h):
        packed = multiply(own_rows[...], h)
        for j in range(per_piece):
            i = j * heads + h
            piece = packed[:, j * height : (j + 1) * height]

            @pl.when(off)
            def _():
                own_parts[i] = piece
                own_copy(i).start()

            @pl.when(away)
            def _():
                parts_a[i] = piece

    def send_far(i):
        top = i // heads * height
        far_parts[i] = multiply(far_rows[:, top : top + height], i % heads)

        @pl.when(off)
        def _():
            far_copy_b(i).start()

        @pl.when(away)
        def _():
            far_copy_a(i).start()

    def take_rows(q):
        rows_moves[q].wait_recv()
        if q == 0:
            scale_move.wait_recv()
        normalize(far_rows, scale_far, q % batches, q // batches * tall, tall)

    taken = early = 0
    later = list(range(chunks + 1))
    while taken < strips:
        c = later.pop(0)
        query_round(c)
        paced = (c + 1) * slots * length * chunk_width // (tall * depth)
        if c == 0:
            weight_local.wait()
            weight_arrives.wait_recv()
        if c < heads:
            own_head(c)
        upto = paced
        if (c + 2) * slots * length * chunk_width >= strips * tall * depth:
            upto = strips
        while taken < upto:
            take_rows(taken)
            taken += 1
        if early < heads and taken * tall >= batches * height:
            send_far(early)
            early += 1

    def kv_copy(way, h):
        return remote(
            kv_out.at[h, way],
            kv_in[h].at[way],
            kv_send.at[h, way],
            kv_recv.at[h, way],
            onward(way),
        )

    def kv_step(way, h):
        @pl.when(has_out(way))
        def _():
            @pl.when(has_in(way))
            def _():
                kv_copy(way, h).wait_recv()

            for j in range(slots):
                own = jnp.where(chosen(1, j, way) > 0, kv_own[h, 1], kv_own[h, 0])
                kv_out[h, way, j] = jnp.where(
                    chosen(0, j, way) > 0, kv_in[h][way, j], own
                )
            kv_copy(way, h).start()

    def join(h):
        @pl.when(off)
        def _():
            far_copy_a(h).wait_recv()

        far_copy_b(h).wait_recv()
        for s in range(batches):
            kv_own[h, s] = pack_parts(
                unpack_parts(parts_a[h, s]) + unpack_parts(parts_b[h, s])
            )

    per_head = chunks // heads
    group = per_head * chunk_width // HEAD_SIZE
    across = (((1,), (1,)), ((), ()))

    def place_of(s):
        want = me * batches + s
        own_at = jnp.int32(-1)
        for b in range(batches):
            for rank in range(ranks):
                hit = (me == rank) & (plan[rank * batches + b] == want)
                own_at = jnp.where(hit, b, own_at)
        in_at = []
        for way in range(2):
            at = jnp.int32(-1)
            for j in range(slots):
                at = jnp.where(routes[way][2][j] == want, j, at)
            in_at.append(at)
        source = jnp.int32(0)
        for b in range(ranks * batches):
            source = jnp.where(plan[b] == want, b, source)
        return own_at, in_at[0], in_at[1], source

    def pick(own, coming, places):
        own_at, right_at, left_at, _ = places
        value = jnp.where(
            right_at >= 0, coming(0, jnp.maximum(right_at, 0)), own(jnp.maximum(own_at, 0))
        )
        return jnp.where(left_at >= 0, coming(1, jnp.maximum(left_at, 0)), value)

    spots = [place_of(s) for s in range(batches)]

    def settle(copy, index):
        for way in range(2):

            @pl.when(has_in(way) & jnp.logical_not(has_out(way)))
            def _():
                copy(way, index).wait_recv()

    def attend_head(h):
        for i in range(h, pieces, heads):
            settle(kv_copy, i)

        @pl.loop(0, batches)
        def _(s):
            places = [jnp.where(s == 0, a, b) for a, b in zip(*spots)]
            tiles = []
            for c in range(h * per_head, (h + 1) * per_head):
                wide = pick(
                    lambda at: query_own[c, at], lambda way, at: query_in[c, way, at], places
                )
                for g in range(chunk_width // HEAD_SIZE):
                    tiles.append(wide[:, g * HEAD_SIZE : (g + 1) * HEAD_SIZE])
            query = jnp.concatenate(tiles, axis=0)
            kv = jnp.concatenate(
                [
                    pick(lambda at: kv_own[i, at], lambda way, at: kv_in[i][way, at], places)
                    for i in range(h, pieces, heads)
                ],
                axis=0,
            )
            value = kv[:, 2 * HEAD_SIZE :]
            line = documents[places[3] // batches, places[3] % batches]
            line = jnp.broadcast_to(line[0:1, :], (length, length))
            query = jnp.concatenate([query, query], axis=1)
            keys = kv[:, : 2 * HEAD_SIZE]
            scores = lax.dot_general(query, keys, across, preferred_element_type=jnp.float32)
            scores = (scores * HEAD_SIZE ** (-0.5)).reshape(group, length, length)
            allowed = (line == line.T) & (columns_of <= rows_of)
            scores = jnp.where(allowed[None], scores, -1e30)
            row_max = jnp.max(scores, axis=-1, keepdims=True)
            expo = jnp.exp(scores - row_max)
            weights = (expo * (1.0 / jnp.sum(expo, axis=-1, keepdims=True))).astype(jnp.bfloat16)
            result = jnp.dot(
                weights.reshape(group * length, length),
                value,
                preferred_element_type=jnp.float32,
            ).astype(jnp.bfloat16)
            top = pl.multiple_of(s * length, length)
            for g in range(group):
                start = (h * group + g) * HEAD_SIZE
                out_ref[pl.ds(top, length), start : start + HEAD_SIZE] = result[
                    g * length : (g + 1) * length
                ]

    def kv_round(i):
        join(i)
        kv_step(first, i)
        if i == 0:
            query_round(later.pop(0))
        if i >= 2:
            kv_step(second_way, i - 2)

    rounds_done = 0
    for i in range(early, pieces):
        send_far(i)
        if i >= heads and len(later) > 1:
            query_round(later.pop(0))
        elif i > heads and len(later) <= 1:
            kv_round(rounds_done)
            rounds_done += 1
    while len(later) > 1:
        query_round(later.pop(0))
    for i in range(rounds_done, pieces):
        kv_round(i)
    for i in range(pieces - 2, pieces):
        kv_step(second_way, i)
    for c in rounds:
        settle(query_copy, c)
    for move in document_arrivals:
        move.wait_recv()
    for h in range(heads):
        attend_head(h)

    for move in rows_moves + [weight_move, stats_move, scale_move] + document_moves:
        move.wait_send()
    for way in range(2):

        @pl.when(has_out(way))
        def _():
            for c in rounds:
                query_copy(way, c).wait_send()
            for i in range(pieces):
                kv_copy(way, i).wait_send()

    for i in range(pieces):

        @pl.when(off)
        def _():
            own_copy(i).wait_send()

        far_copy_a(i).wait_send()


def fused(slots, plan, tokens, queries, segment_ids, gain, key_value_weight):
    ranks = lax.axis_size("dp")
    batches, length = segment_ids.shape
    rows, depth = tokens.shape
    width = queries.shape[1]
    heads = 2 * key_value_weight.shape[1] // (2 * HEAD_SIZE)
    chunks = 4 * heads
    chunk_width = width // chunks
    pieces = 2 * heads
    packed = (length // 2, 3 * HEAD_SIZE)
    bf16, f32 = jnp.bfloat16, jnp.float32
    limit = (5 + slots) * 6 * 2**20
    dma = pltpu.SemaphoreType.DMA
    anywhere = pl.BlockSpec(memory_space=pl.ANY)
    return pl.pallas_call(
        functools.partial(fused_kernel, slots),
        out_shape=jax.ShapeDtypeStruct((rows, width), bf16),
        in_specs=[
            pl.BlockSpec(memory_space=pltpu.SMEM),
            anywhere,
            anywhere,
            pl.BlockSpec(memory_space=pltpu.VMEM),
            pl.BlockSpec(memory_space=pltpu.VMEM),
            anywhere,
        ],
        out_specs=pl.BlockSpec(memory_space=pltpu.VMEM),
        scratch_shapes=[
            pltpu.VMEM((batches, length, depth), bf16),
            pltpu.VMEM((batches, length, depth), bf16),
            pltpu.VMEM((2, depth, key_value_weight.shape[1]), bf16),
            pltpu.VMEM((batches, 8, length), f32),
            pltpu.VMEM((batches, 8, length), f32),
            pltpu.VMEM((batches, 8, length), f32),
            pltpu.VMEM((batches, 8, length), f32),
            pltpu.VMEM((chunks, batches, length, chunk_width), bf16),
            pltpu.VMEM((chunks, 2, slots, length, chunk_width), bf16),
            pltpu.VMEM((chunks, 2, slots, length, chunk_width), bf16),
            pltpu.VMEM((ranks, batches, 8, length), f32),
            pltpu.VMEM((pieces, batches, *packed), bf16),
            pltpu.VMEM((pieces, batches, *packed), bf16),
            pltpu.VMEM((pieces, batches, *packed), bf16),
            pltpu.VMEM((pieces, batches, *packed), bf16),
            pltpu.VMEM((pieces, batches, *packed), bf16),
            pltpu.VMEM((pieces, 2, slots, *packed), bf16),
        ]
        + [pltpu.VMEM((2, slots, *packed), bf16)] * pieces
        + [
            dma,
            dma,
            dma((chunks,)),
            dma((4 * batches,)),
            dma((4 * batches,)),
            dma,
            dma,
            dma,
            dma,
            dma,
            dma,
            dma((chunks, 2)),
            dma((chunks, 2)),
            dma((ranks - 1,)),
            dma((ranks - 1,)),
            dma((pieces,)),
            dma((pieces,)),
            dma((pieces,)),
            dma((pieces,)),
            dma((pieces, 2)),
            dma((pieces, 2)),
        ],
        compiler_params=pltpu.CompilerParams(
            collective_id=slots, has_side_effects=True, vmem_limit_bytes=limit
        ),
        name="fused",
    )(
        plan,
        tokens.reshape(batches, length, depth),
        queries.reshape(batches, length, width),
        segment_ids,
        gain.reshape(1, depth),
        key_value_weight,
    )


def fused_shards(tokens, queries, segment_ids, gain, key_value_weight, plan):
    ranks = lax.axis_size("dp")
    batches = segment_ids.shape[0]
    most = batches * (ranks // 2)
    branches = [functools.partial(fused, slots) for slots in range(batches, most + 1)]
    source = np.arange(plan.shape[0]) // batches
    crossing = [
        jnp.sum(jnp.where(source < cut, plan >= cut * batches, False).astype(jnp.int32))
        for cut in range(2, ranks - 1)
    ]
    index = jnp.clip(functools.reduce(jnp.maximum, crossing, batches) - batches, 0, most - batches)
    return lax.switch(
        index, branches, plan, tokens, queries, segment_ids, gain, key_value_weight
    )


def solution(mesh):
    placed = (
        P(("dp", "fsdp"), "tensor"),
        P(("dp", "fsdp"), "tensor"),
        P(("dp", "fsdp"), None),
        P("tensor"),
        P("tensor", "fsdp"),
        P(),
    )
    small = mesh.shape["tensor"] == 2 and mesh.shape["fsdp"] == 4 and mesh.shape["dp"] <= 4
    return jax.shard_map(
        fused_shards if small else shards,
        mesh=mesh,
        in_specs=placed,
        out_specs=P(("dp", "fsdp"), "tensor"),
        check_vma=False,
    )
```
